8 devices in a mesh: rep: 4 (over z, y, x), fsdp: 2 (over core).
Axes of the slice: x: 2, y: 2, z: 1, core: 2. Of those that a mesh axis runs over, the one named last changes fastest.
Arguments:
- tokens: int32 [256, 32], P(('rep', 'fsdp'))
- resp_mask: int32 [256, 32], P(('rep', 'fsdp'))
- logp_old: float32 [256, 32], P(('rep', 'fsdp'))
- rewards: float32 [256], P(('rep', 'fsdp'))
- group_id: int32 [256], P(('rep', 'fsdp'))
- pol_wq: bfloat16 [2, 1600, 1600], P(None, 'fsdp')
- pol_wkv: bfloat16 [2, 1600, 640], P(None, 'fsdp')
- pol_wo: bfloat16 [2, 1600, 1600], P(None, 'fsdp')
- pol_wgu: bfloat16 [2, 1600, 8704], P(None, 'fsdp')
- pol_wdown: bfloat16 [2, 4352, 1600], P(None, 'fsdp')
- pol_norms: bfloat16 [5, 1600], P(None, 'fsdp')
- pol_embed: bfloat16 [32000, 1600], P('fsdp')
- pol_head: bfloat16 [32000, 1600], P('fsdp')
- ref_wq: bfloat16 [2, 1600, 1600], P(None, ('rep', 'fsdp'))
- ref_wkv: bfloat16 [2, 1600, 640], P(None, ('rep', 'fsdp'))
- ref_wo: bfloat16 [2, 1600, 1600], P(None, ('rep', 'fsdp'))
- ref_wgu: bfloat16 [2, 1600, 8704], P(None, ('rep', 'fsdp'))
- ref_wdown: bfloat16 [2, 4352, 1600], P(None, ('rep', 'fsdp'))
- ref_norms: bfloat16 [5, 1600], P(None, ('rep', 'fsdp'))
- ref_embed: bfloat16 [32000, 1600], P(('rep', 'fsdp'))
- ref_head: bfloat16 [32000, 1600], P(('rep', 'fsdp'))
Outputs:
- output 1: float32 [], replicated
- output 2: float32 [256, 32], P(('rep', 'fsdp'))
- output 3: float32 [256, 32], P(('rep', 'fsdp'))
All inputs are finite; a program needn't handle non-finite values.
Results may differ from the reference program's by a relative error of at most 0.00177.
Values are sent between devices in bfloat16 or wider.
A program may use at most 1 GiB of HBM per device.

```python
import math
import jax
import jax.numpy as jnp
from jax import lax

D = 1600
HEADS = 25
KV_HEADS = 5
HEAD = 64
FF = 4352
VOCAB = 32000
LAYERS = 2
ROWS_DEV = 32
SEQ = 32
BATCH = 256
GROUP = 8

REP_Q = HEADS // KV_HEADS
NUM_GROUPS = BATCH // GROUP
EPS = 1e-6
ROPE_BASE = 10000.0
CLIP_EPS = 0.2
BETA = 0.04
ADV_EPS = 1e-4
MODEL_NAMES = ['wq', 'wkv', 'wo', 'wgu', 'wdown', 'norms', 'embed', 'head']


def draw_matrix(key, shape, fan_in):
    return (jax.random.normal(key, shape, jnp.float32) * fan_in ** -0.5).astype(jnp.bfloat16)


def draw_model(key):
    keys = jax.random.split(key, 8)
    w_q = draw_matrix(keys[0], (LAYERS, D, HEADS * HEAD), D)
    w_kv = draw_matrix(keys[1], (LAYERS, D, 2 * KV_HEADS * HEAD), D)
    w_o = draw_matrix(keys[2], (LAYERS, HEADS * HEAD, D), HEADS * HEAD)
    w_gu = draw_matrix(keys[3], (LAYERS, D, 2 * FF), D)
    w_down = draw_matrix(keys[4], (LAYERS, FF, D), FF)
    norms = (1.0 + 0.3 * jax.random.normal(keys[5], (2 * LAYERS + 1, D), jnp.float32)).astype(jnp.bfloat16)
    embed = jax.random.normal(keys[6], (VOCAB, D), jnp.float32).astype(jnp.bfloat16)
    head = draw_matrix(keys[7], (VOCAB, D), 4 * D)
    return [w_q, w_kv, w_o, w_gu, w_down, norms, embed, head]


def draw_layout(key):
    key_prompt, key_resp, key_perm = jax.random.split(key, 3)
    prompt_len = jax.random.randint(key_prompt, (BATCH, 1), 1, SEQ // 2 + 1)
    resp_len = jax.random.randint(key_resp, (BATCH, 1), 1, SEQ - prompt_len + 1)
    positions = jnp.arange(SEQ)[None, :]
    resp_mask = ((positions >= prompt_len) & (positions < prompt_len + resp_len)).astype(jnp.int32)
    group_id = jax.random.permutation(key_perm, jnp.arange(BATCH, dtype=jnp.int32) // GROUP)
    return resp_mask, group_id


def setup_inputs(seed: int = 0) -> dict:
    key_pol, key_ref, key_layout, key_tok, key_old, key_rew = jax.random.split(jax.random.key(seed), 6)
    resp_mask, group_id = draw_layout(key_layout)
    inputs = {}
    inputs['tokens'] = jax.random.randint(key_tok, (BATCH, SEQ), 0, VOCAB, dtype=jnp.int32)
    inputs['resp_mask'] = resp_mask
    inputs['logp_old'] = -math.log(VOCAB) - 0.125 + 0.3 * jax.random.normal(key_old, (BATCH, SEQ), jnp.float32)
    inputs['rewards'] = jax.random.normal(key_rew, (BATCH,), jnp.float32)
    inputs['group_id'] = group_id
    for name, array_val in zip(MODEL_NAMES, draw_model(key_pol)):
        inputs['pol_' + name] = array_val
    for name, array_val in zip(MODEL_NAMES, draw_model(key_ref)):
        inputs['ref_' + name] = array_val
    return inputs


def rms_norm(hidden, gain):
    hidden_f32 = hidden.astype(jnp.float32)
    inv_rms = lax.rsqrt(jnp.mean(hidden_f32 * hidden_f32, axis=-1, keepdims=True) + EPS)
    return (hidden_f32 * inv_rms * gain.astype(jnp.float32)).astype(jnp.bfloat16)


def rope_tables():
    half = HEAD // 2
    inv_freq = ROPE_BASE ** (-jnp.arange(half, dtype=jnp.float32) / half)
    angles = jnp.arange(SEQ, dtype=jnp.float32)[:, None] * inv_freq[None, :]
    return jnp.cos(angles)[None, :, None, :], jnp.sin(angles)[None, :, None, :]


def apply_rope(vec_f32, cos_tab, sin_tab):
    half = HEAD // 2
    first = vec_f32[..., :half]
    second = vec_f32[..., half:]
    return jnp.concatenate([first * cos_tab - second * sin_tab, second * cos_tab + first * sin_tab], axis=-1)


def decoder_layer(hidden, params, cos_tab, sin_tab):
    layer_q, layer_kv, layer_o, layer_gu, layer_down, gain_attn, gain_mlp = params
    rows = hidden.shape[0]
    normed = rms_norm(hidden, gain_attn).reshape(rows * SEQ, D)
    query = jnp.dot(normed, layer_q, preferred_element_type=jnp.float32).reshape(rows, SEQ, HEADS, HEAD)
    key_val = jnp.dot(normed, layer_kv, preferred_element_type=jnp.float32).reshape(rows, SEQ, 2, KV_HEADS, HEAD)
    q_rot = apply_rope(query, cos_tab, sin_tab).astype(jnp.bfloat16).reshape(rows, SEQ, KV_HEADS, REP_Q, HEAD)
    k_rot = apply_rope(key_val[:, :, 0], cos_tab, sin_tab).astype(jnp.bfloat16)
    v_val = key_val[:, :, 1].astype(jnp.bfloat16)
    scores = jnp.einsum('bqkrd,bskd->bkrqs', q_rot.astype(jnp.float32), k_rot.astype(jnp.float32)) * HEAD ** -0.5
    causal = jnp.arange(SEQ)[:, None] >= jnp.arange(SEQ)[None, :]
    scores = jnp.where(causal, scores, -1e30)
    attn_prob = jax.nn.softmax(scores, axis=-1).astype(jnp.bfloat16)
    attn_out = jnp.einsum('bkrqs,bskd->bqkrd', attn_prob.astype(jnp.float32), v_val.astype(jnp.float32)).astype(jnp.bfloat16)
    attn_proj = jnp.dot(attn_out.reshape(rows * SEQ, HEADS * HEAD), layer_o, preferred_element_type=jnp.float32)
    hidden = (hidden.astype(jnp.float32) + attn_proj.reshape(rows, SEQ, D)).astype(jnp.bfloat16)
    normed = rms_norm(hidden, gain_mlp).reshape(rows * SEQ, D)
    gate_up = jnp.dot(normed, layer_gu, preferred_element_type=jnp.float32)
    swiglu = (jax.nn.silu(gate_up[:, :FF]) * gate_up[:, FF:]).astype(jnp.bfloat16)
    down = jnp.dot(swiglu, layer_down, preferred_element_type=jnp.float32)
    return (hidden.astype(jnp.float32) + down.reshape(rows, SEQ, D)).astype(jnp.bfloat16)


def model_logprobs(tokens, model):
    w_q, w_kv, w_o, w_gu, w_down, norms, embed, head = model
    rows = tokens.shape[0]
    cos_tab, sin_tab = rope_tables()
    hidden = jnp.take(embed, tokens, axis=0)

    def layer_step(carry, params):
        return decoder_layer(carry, params, cos_tab, sin_tab), None

    stacked = (w_q, w_kv, w_o, w_gu, w_down, norms[0:2 * LAYERS:2], norms[1:2 * LAYERS:2])
    hidden = lax.scan(layer_step, hidden, stacked)[0]
    normed = rms_norm(hidden, norms[2 * LAYERS]).reshape(rows * SEQ, D)
    logits = jnp.dot(normed, head.T, preferred_element_type=jnp.float32).reshape(rows, SEQ, VOCAB)
    targets = jnp.roll(tokens, -1, axis=1)
    picked = jnp.take_along_axis(logits, targets[:, :, None], axis=-1)[:, :, 0]
    next_lp = picked - jax.nn.logsumexp(logits, axis=-1)
    col_index = jnp.arange(SEQ)[None, :]
    return jnp.where(col_index == 0, 0.0, jnp.roll(next_lp, 1, axis=1))


def advantages(rewards, group_id):
    means = jax.ops.segment_sum(rewards, group_id, num_segments=NUM_GROUPS) / GROUP
    centred = rewards - means[group_id]
    spread = jnp.sqrt(jax.ops.segment_sum(centred * centred, group_id, num_segments=NUM_GROUPS) / GROUP)
    return centred / (spread[group_id] + ADV_EPS)


def row_losses(logp, logp_ref, logp_old, resp_mask, advantage):
    log_gap = logp_ref - logp
    kl_est = jnp.exp(log_gap) - log_gap - 1.0
    ratio = jnp.exp(logp - logp_old)
    adv_row = advantage[:, None]
    surrogate = jnp.minimum(ratio * adv_row, jnp.clip(ratio, 1.0 - CLIP_EPS, 1.0 + CLIP_EPS) * adv_row)
    per_token = -surrogate + BETA * kl_est
    weights = resp_mask.astype(jnp.float32)
    return jnp.sum(per_token * weights, axis=1) / jnp.sum(weights, axis=1)


def reference(tokens, resp_mask, logp_old, rewards, group_id, pol_wq, pol_wkv, pol_wo, pol_wgu, pol_wdown, pol_norms, pol_embed, pol_head, ref_wq, ref_wkv, ref_wo, ref_wgu, ref_wdown, ref_norms, ref_embed, ref_head):
    policy = (pol_wq, pol_wkv, pol_wo, pol_wgu, pol_wdown, pol_norms, pol_embed, pol_head)
    frozen = (ref_wq, ref_wkv, ref_wo, ref_wgu, ref_wdown, ref_norms, ref_embed, ref_head)

    def block_logprobs(block_tokens):
        return model_logprobs(block_tokens, policy), model_logprobs(block_tokens, frozen)

    blocks = tokens.reshape(BATCH // ROWS_DEV, ROWS_DEV, SEQ)
    pol_blocks, ref_blocks = lax.map(block_logprobs, blocks)
    logp = pol_blocks.reshape(BATCH, SEQ)
    logp_ref = ref_blocks.reshape(BATCH, SEQ)
    advantage = advantages(rewards, group_id)
    loss = jnp.mean(row_losses(logp, logp_ref, logp_old, resp_mask, advantage))
    return loss, logp, logp_ref
```

```python
import functools

import jax
import jax.numpy as jnp
from jax import lax
from jax.experimental import pallas as pl
from jax.experimental.pallas import tpu as pltpu
from jax.sharding import PartitionSpec as P

HEAD_DIM = 64
EPS = 1e-6
ROPE_BASE = 10000.0
CLIP_EPS = 0.2
BETA = 0.04
ADV_EPS = 1e-4

F32 = jnp.float32
BF16 = jnp.bfloat16
NEG = -3.0e38
VMEM_LIMIT = 62 * 1024 * 1024

D = 1600
QH = 25
KVH = 5
QKV = 2240
FF = 4352
SEQ = 32
TB = 256
SUB = 128
FT = 256
VT = 2048


def dot(lhs, rhs):
    return lax.dot_general(lhs, rhs, (((1,), (0,)), ((), ())), preferred_element_type=F32)


def dot_nt(lhs, rhs):
    return lax.dot_general(lhs, rhs, (((1,), (1,)), ((), ())), preferred_element_type=F32)


def rms(x, gain):
    x = x.astype(F32)
    inv = lax.rsqrt(jnp.sum(x * x, axis=-1, keepdims=True) * (1.0 / D) + EPS)
    return (x * inv * gain).astype(BF16)


def row_copies(parts, layer, half_of, dst, sems, base):
    out = []
    for p, part in enumerate(parts):
        src = part if layer is None else part.at[layer]
        rows = src.shape[0]
        at = pl.multiple_of(half_of(p) * rows, 8) if len(parts) > 1 else 0
        out.append(pltpu.make_async_copy(src, dst.at[pl.ds(at, rows)], sems.at[base + p]))
    return out


def attn_kernel(n, layer, core_ref, h_ref, gain_ref, cos_ref, sin_ref, *refs):
    qkv_parts, wo_parts = refs[:n], refs[n:2 * n]
    out_ref, wqkv, wo, qkv_s, qk_s, o_s, sc_s, p_s, sems = refs[2 * n:]
    core = core_ref[0]

    def half_of(p):
        return jnp.bitwise_xor(core, p)

    first = row_copies(qkv_parts, layer, half_of, wqkv, sems, 0)
    second = row_copies(wo_parts, layer, half_of, wo, sems, n)
    for copy in first + second:
        copy.start()
    for copy in first:
        copy.wait()

    lane = lax.broadcasted_iota(jnp.int32, (1, 128), 1)
    low_half = lane < 64
    rot_mask = (lane % 64) < 32
    q_idx = lax.broadcasted_iota(jnp.int32, (SUB, 2 * SUB), 0)
    k_idx = lax.broadcasted_iota(jnp.int32, (SUB, 2 * SUB), 1) % SUB
    keep = (q_idx // SEQ == k_idx // SEQ) & (k_idx <= q_idx)
    zero = jnp.zeros((), BF16)

    def project(b):
        rows = pl.ds(pl.multiple_of(b * TB, TB), TB)
        qkv_s[...] = dot(rms(h_ref[rows, :], gain_ref[...]), wqkv[...])
        cos, sin = cos_ref[...], sin_ref[...]
        for j in range(15):
            x = qkv_s[:, 128 * j:128 * (j + 1)]
            rot = jnp.where(rot_mask, pltpu.roll(x, 96, 1), pltpu.roll(x, 32, 1))
            qk_s[:, 128 * j:128 * (j + 1)] = (x * cos + rot * sin).astype(BF16)

    def attend(s):
        rows = slice(s * SUB, (s + 1) * SUB)
        k_pads, v_pads = [], []
        for g in range(KVH):
            c, side = divmod(25 + g, 2)
            x = qk_s[rows, 128 * c:128 * (c + 1)].astype(F32)
            y = pltpu.roll(x, 64, 1)
            at_low, at_high = (y, x) if side else (x, y)
            k_pads.append((jnp.where(low_half, at_low, 0.0).astype(BF16), jnp.where(low_half, 0.0, at_high).astype(BF16)))
            c, side = divmod(g, 2)
            if c < 2:
                x = qkv_s[rows, 1920 + 128 * c:2048 + 128 * c]
            else:
                x = jnp.concatenate([qkv_s[rows, 2176:2240], jnp.zeros((SUB, 64), F32)], axis=1)
            y = pltpu.roll(x, 64, 1)
            at_low, at_high = (y, x) if side else (x, y)
            v_pads.append((jnp.where(low_half, at_low, 0.0).astype(BF16), jnp.where(low_half, 0.0, at_high).astype(BF16)))
        heads = [((2 * j) // 5, min((2 * j + 1) // 5, KVH - 1)) for j in range(13)]
        for j, (ga, gb) in enumerate(heads):
            keys = jnp.concatenate([k_pads[ga][0], k_pads[gb][1]], axis=0)
            scores = dot_nt(qk_s[rows, 128 * j:128 * (j + 1)], keys) * (HEAD_DIM ** -0.5)
            sc_s[:, 2 * SUB * j:2 * SUB * (j + 1)] = jnp.where(keep, scores, -1e30)
        for i in range(QH):
            x = sc_s[:, SUB * i:SUB * (i + 1)]
            e = jnp.exp(x - jnp.max(x, axis=1, keepdims=True))
            p_s[:, SUB * i:SUB * (i + 1)] = (e * (1.0 / jnp.sum(e, axis=1, keepdims=True))).astype(BF16)
        for j, (ga, gb) in enumerate(heads):
            if j < 12:
                vals = jnp.concatenate([v_pads[ga][0], v_pads[gb][1]], axis=0)
                o_s[rows, 128 * j:128 * (j + 1)] = dot(p_s[:, 2 * SUB * j:2 * SUB * (j + 1)], vals).astype(BF16)
            else:
                o_s[rows, 1536:1600] = dot(p_s[:, 2 * SUB * j:2 * SUB * j + SUB], v_pads[ga][0]).astype(BF16)[:, :64]

    def block(b, carry):
        rows = pl.ds(pl.multiple_of(b * TB, TB), TB)
        project(b)
        for s in range(TB // SUB):
            attend(s)

        @pl.when(b == 0)
        def _():
            for copy in second:
                copy.wait()

        out_ref[rows, :] = (h_ref[rows, :].astype(F32) + dot(o_s[...], wo[...])).astype(BF16)
        return carry

    lax.fori_loop(0, h_ref.shape[0] // TB, block, 0)


def attention_block(h, gain, tabs, w_qkv, w_o, layer, core):
    n = len(w_qkv)
    t = h.shape[0]
    vm = pl.BlockSpec(memory_space=pltpu.VMEM)
    anym = pl.BlockSpec(memory_space=pl.ANY)
    return pl.pallas_call(
        functools.partial(attn_kernel, n, layer),
        out_shape=jax.ShapeDtypeStruct((t, D), BF16),
        in_specs=[pl.BlockSpec(memory_space=pltpu.SMEM), vm, vm, vm, vm] + [anym] * (2 * n),
        out_specs=vm,
        scratch_shapes=[
            pltpu.VMEM((D, QKV), BF16), pltpu.VMEM((D, D), BF16), pltpu.VMEM((TB, QKV), F32),
            pltpu.VMEM((TB, 1920), BF16), pltpu.VMEM((TB, D), BF16), pltpu.VMEM((SUB, 26 * SUB), F32), pltpu.VMEM((SUB, 26 * SUB), BF16),
            pltpu.SemaphoreType.DMA((2 * n,)),
        ],
        compiler_params=pltpu.CompilerParams(vmem_limit_bytes=VMEM_LIMIT),
        cost_estimate=pl.CostEstimate(flops=2 * t * D * (QKV + D), bytes_accessed=2 * D * (QKV + D), transcendentals=0),
        name="attn",
    )(core, h, gain, tabs[0], tabs[1], *w_qkv, *w_o)


def mlp_kernel(n, layer, last, core_ref, h_ref, gain_ref, fin_ref, *refs):
    gu_parts, dn_parts = refs[:n], refs[n:2 * n]
    out_ref, wg, wu, wd, c_s, act_s, acc, sems, dn_sems = refs[2 * n:]
    core = core_ref[0]
    steps = FF // FT
    half_subs = FF // 2 // 128

    def gu_copies(j, slot):
        out = []
        for p, part in enumerate(gu_parts):
            src = part if layer is None else part.at[layer]
            rows = src.shape[0]
            at = pl.multiple_of(jnp.bitwise_xor(core, p) * rows, 8) if n > 1 else 0
            for t, dst in enumerate((wg, wu)):
                cols = pl.ds(pl.multiple_of(t * FF + j * FT, 128), FT)
                out.append(pltpu.make_async_copy(src.at[:, cols], dst.at[slot, pl.ds(at, rows)], sems.at[slot, 2 * p + t]))
        return out

    def dn_copy(part, j, i):
        slot = lax.rem(j, 3)
        src = part if layer is None else part.at[layer]
        if n == 1:
            at = pl.multiple_of(j * FT, FT)
            return pltpu.make_async_copy(src.at[pl.ds(at, FT)], wd.at[slot], dn_sems.at[slot, 0])
        sub = 2 * j + i
        col = pl.multiple_of(jnp.where(sub >= half_subs, sub - half_subs, sub) * 128, 128)
        return pltpu.make_async_copy(src.at[:, pl.ds(col, 128)], wd.at[slot, :, pl.ds(128 * i, 128)], dn_sems.at[slot, i])

    def start(j):
        for copy in gu_copies(j, lax.rem(j, 2)):
            copy.start()
        if n == 1:
            dn_copy(dn_parts[0], j, 0).start()
        else:
            for i in range(2):
                half = (2 * j + i >= half_subs).astype(jnp.int32)
                mine = half == core

                @pl.when(mine)
                def _():
                    dn_copy(dn_parts[0], j, i).start()

                @pl.when(jnp.logical_not(mine))
                def _():
                    dn_copy(dn_parts[1], j, i).start()

    def wait_gu(j):
        for copy in gu_copies(j, lax.rem(j, 2)):
            copy.wait()

    def wait_dn(j):
        for i in range(n):
            dn_copy(dn_parts[0], j, i).wait()

    def gate_up(j):
        slot = lax.rem(j, 2)
        g = dot(c_s[...], wg[slot])
        u = dot(c_s[...], wu[slot])
        act_s[slot] = (g * jax.nn.sigmoid(g) * u).astype(BF16)

    def down(j):
        act, w = act_s[lax.rem(j, 2)], wd[lax.rem(j, 3)]
        acc[...] += dot(act, w) if n == 1 else dot_nt(act, w)

    zero = jnp.int32(0)
    start(zero)
    start(zero + 1)
    c_s[...] = rms(h_ref[...], gain_ref[...])
    acc[...] = h_ref[...].astype(F32)
    wait_gu(zero)
    gate_up(zero)

    def step(j, carry):
        @pl.when(j + 1 < steps)
        def _():
            start(j + 1)

        wait_gu(j)
        wait_dn(j - 1)
        gate_up(j)
        down(j - 1)
        return carry

    lax.fori_loop(1, steps, step, 0)
    wait_dn(zero + (steps - 1))
    down(zero + (steps - 1))
    out = acc[...].astype(BF16)
    out_ref[...] = rms(out, fin_ref[...]) if last else out


def mlp_block(h, gain, fin, w_gu, w_dn, layer, last, core):
    n = len(w_gu)
    t = h.shape[0]
    vm = pl.BlockSpec(memory_space=pltpu.VMEM)
    anym = pl.BlockSpec(memory_space=pl.ANY)
    return pl.pallas_call(
        functools.partial(mlp_kernel, n, layer, last),
        out_shape=jax.ShapeDtypeStruct((t, D), BF16),
        in_specs=[pl.BlockSpec(memory_space=pltpu.SMEM), vm, vm, vm] + [anym] * (2 * n),
        out_specs=vm,
        scratch_shapes=[
            pltpu.VMEM((2, D, FT), BF16), pltpu.VMEM((2, D, FT), BF16), pltpu.VMEM((3, FT, D) if n == 1 else (3, D, FT), BF16),
            pltpu.VMEM((t, D), BF16), pltpu.VMEM((2, t, FT), BF16), pltpu.VMEM((t, D), F32),
            pltpu.SemaphoreType.DMA((2, 4)), pltpu.SemaphoreType.DMA((3, 2)),
        ],
        compiler_params=pltpu.CompilerParams(vmem_limit_bytes=VMEM_LIMIT),
        cost_estimate=pl.CostEstimate(flops=6 * t * D * FF, bytes_accessed=6 * D * FF, transcendentals=0),
        name="mlp",
    )(core, h, gain, fin, *w_gu, *w_dn)


def head_kernel(vocab, x_ref, w_ref, tgt_ref, out_ref, m_s, s_s, p_s):
    j = pl.program_id(1)

    @pl.when(j == 0)
    def _():
        m_s[...] = jnp.full(m_s.shape, NEG, F32)
        s_s[...] = jnp.zeros(s_s.shape, F32)
        p_s[...] = jnp.zeros(p_s.shape, F32)

    lane = lax.broadcasted_iota(jnp.int32, m_s.shape, 1)
    rel = tgt_ref[...] - lane - j * VT
    held = vocab - j * VT
    for at in range(0, VT, 256):
        logits = dot(x_ref[...], w_ref[:, at:at + 256])
        cols = [logits[:, :128], logits[:, 128:]]
        if at + 256 > (vocab % VT or VT):
            cols = [jnp.where(lane < held - at - 128 * c, x, NEG) for c, x in enumerate(cols)]
        m_old = m_s[...]
        m_new = jnp.maximum(m_old, jnp.maximum(cols[0], cols[1]))
        s_s[...] = s_s[...] * jnp.exp(m_old - m_new) + (jnp.exp(cols[0] - m_new) + jnp.exp(cols[1] - m_new))
        m_s[...] = m_new
        p_s[...] += jnp.where(rel == at, cols[0], jnp.where(rel == at + 128, cols[1], 0.0))

    @pl.when(j == pl.num_programs(1) - 1)
    def _():
        m = m_s[...]
        top = jnp.max(m, axis=1, keepdims=True)
        lse = top + jnp.log(jnp.sum(s_s[...] * jnp.exp(m - top), axis=1, keepdims=True))
        picked = jnp.sum(p_s[...], axis=1, keepdims=True)
        out_ref[...] = jnp.where(lane == 0, lse, picked)


def head_block(x, w, tgt, tt=1024):
    t, v = x.shape[0], w.shape[1]
    tgt = jnp.broadcast_to(jnp.where((tgt >= 0) & (tgt < v), tgt, -1)[:, None], (t, 128))
    out = pl.pallas_call(
        functools.partial(head_kernel, v),
        out_shape=jax.ShapeDtypeStruct((t, 128), F32),
        grid=(t // tt, pl.cdiv(v, VT)),
        in_specs=[
            pl.BlockSpec((tt, D), lambda i, j: (i, 0)), pl.BlockSpec((D, VT), lambda i, j: (0, j)),
            pl.BlockSpec((tt, 128), lambda i, j: (i, 0)),
        ],
        out_specs=pl.BlockSpec((tt, 128), lambda i, j: (i, 0)),
        scratch_shapes=[pltpu.VMEM((tt, 128), F32)] * 3,
        compiler_params=pltpu.CompilerParams(vmem_limit_bytes=VMEM_LIMIT),
        cost_estimate=pl.CostEstimate(flops=2 * t * D * v, bytes_accessed=2 * D * (v * t // tt + t), transcendentals=t * v),
        name="head",
    )(x, w, tgt)
    return out[:, 0], out[:, 1]


def rope_tables():
    half = HEAD_DIM // 2
    inv_freq = ROPE_BASE ** (-jnp.arange(half, dtype=F32) / half)
    angles = jnp.arange(SEQ, dtype=F32)[:, None] * inv_freq[None, :]
    cos, sin = jnp.cos(angles), jnp.sin(angles)
    cos = jnp.tile(jnp.concatenate([cos, cos] * 2, axis=1), (TB // SEQ, 1))
    sin = jnp.tile(jnp.concatenate([-sin, sin] * 2, axis=1), (TB // SEQ, 1))
    return cos, sin


def running_count(flags):
    n = flags.shape[-1]
    upper = (jnp.arange(n)[:, None] <= jnp.arange(n)[None, :]).astype(BF16)
    return dot(flags.astype(BF16), upper).astype(jnp.int32)


def embed_rows(table, toks, me, size, cap, perms, axis, order):
    vocab, t = table.shape[0], toks.shape[1]
    local = toks - me * vocab
    owned = (local >= 0) & (local < vocab)
    rank = running_count(owned) - 1
    peers = jnp.bitwise_xor(me, jnp.arange(size))
    wanted = (toks[0] // vocab)[None, :] == peers[:, None]
    my_rank = running_count(wanted) - 1

    def one_round(r):
        slots = r * cap + jnp.arange(cap)
        hit = owned[:, None, :] & (rank[:, None, :] == slots[None, :, None])
        idx = jnp.sum(jnp.where(hit, local[:, None, :], 0), axis=2)
        got = [jnp.take(table, idx[0], axis=0)]
        rows = jnp.take(table, idx[1:].reshape(-1), axis=0).reshape(size - 1, cap, D)
        for k in range(1, size):
            got.append(lax.ppermute(rows[k - 1], axis, perms[k]))
        pick = wanted[:, :, None] & (my_rank[:, :, None] == slots[None, None, :])
        pick = jnp.swapaxes(pick, 0, 1).reshape(t, size * cap).astype(BF16)
        return dot(pick, jnp.concatenate(got, axis=0))

    counts = jnp.sum((order[:, None, :] // vocab) == jnp.arange(32000 // vocab)[None, :, None], axis=2)
    rounds = (jnp.max(counts) + cap - 1) // cap
    rows = one_round(0)
    rows = lax.fori_loop(1, rounds, lambda r, acc: acc + one_round(r), rows)
    return rows.astype(BF16)


def advantages(rewards, groups):
    same = (groups[:, None] == groups[None, :]).astype(F32)
    counts = jnp.sum(same, axis=1)
    means = jnp.sum(same * rewards[None, :], axis=1) / counts
    centred = rewards - means
    spread = jnp.sqrt(jnp.sum(same * (centred * centred)[None, :], axis=1) / counts)
    return centred / (spread + ADV_EPS)


def row_losses(logp, logp_ref, logp_old, weights, advantage):
    log_gap = logp_ref - logp
    kl_est = jnp.exp(log_gap) - log_gap - 1.0
    ratio = jnp.exp(logp - logp_old)
    adv_row = advantage[:, None]
    surrogate = jnp.minimum(ratio * adv_row, jnp.clip(ratio, 1.0 - CLIP_EPS, 1.0 + CLIP_EPS) * adv_row)
    per_token = -surrogate + BETA * kl_est
    return jnp.sum(per_token * weights, axis=1) / jnp.sum(weights, axis=1)


def solution(mesh):
    both = ('rep', 'fsdp')
    row_spec = P(both, None)
    n_dev = mesh.shape['rep'] * mesh.shape['fsdp']
    swap = [(0, 1), (1, 0)]
    xors = [[(d, d ^ k) for d in range(n_dev)] for k in range(n_dev)]

    def weight_specs(axes):
        return [P(None, axes, None)] * 5 + [P(None, axes), P(axes, None), P(axes, None)]

    in_specs = tuple([row_spec, row_spec, row_spec, P(both), P(both)] + weight_specs('fsdp') + weight_specs(both))
    out_specs = (P(), row_spec, row_spec)

    def device_step(tokens, resp_mask, logp_old, rewards, group_id, *weights):
        p_q, p_kv, p_o, p_gu, p_dn, p_norms, p_embed, p_head = weights[:8]
        r_q, r_kv, r_o, r_gu, r_dn, r_norms, r_embed, r_head = weights[8:]
        core = lax.axis_index('fsdp')
        me = lax.axis_index('rep') * 2 + core
        core_arr = core.astype(jnp.int32).reshape(1)
        rows = tokens.shape[0]
        t = rows * SEQ
        layers = p_q.shape[0]
        tabs = rope_tables()

        small = jnp.concatenate([x.astype(F32).reshape(-1) for x in (tokens, resp_mask, logp_old, rewards, group_id, p_norms, r_norms)])
        size = -small.size % 1024
        small = lax.all_gather(jnp.pad(small, (0, size)).reshape(-1, 128), both).reshape(n_dev, -1)
        cuts, at = [], 0
        for x in (tokens, resp_mask, logp_old, rewards, group_id, p_norms, r_norms):
            cuts.append(small[:, at:at + x.size].reshape((n_dev,) + x.shape))
            at += x.size
        tok_all = cuts[0].astype(jnp.int32).reshape(n_dev, t)
        mask_all, old_all = (x.reshape(n_dev * rows, SEQ) for x in cuts[1:3])
        reward_all = cuts[3].reshape(-1)
        group_all = cuts[4].reshape(-1)
        p_gains = jnp.swapaxes(cuts[5][:2], 0, 1).reshape(2 * layers + 1, 1, D)
        r_gains = jnp.swapaxes(cuts[6], 0, 1).reshape(2 * layers + 1, 1, D)
        tgt_all = jnp.roll(tok_all.reshape(n_dev * rows, SEQ), -1, axis=1).reshape(n_dev, t)

        p_qkv = jnp.concatenate([p_q, p_kv], axis=2)
        p_qkv, p_wo, p_wgu, p_wdn = ([w, lax.ppermute(w, 'fsdp', swap)] for w in (p_qkv, p_o, p_gu, jnp.swapaxes(p_dn, 1, 2)))
        p_head, r_head = p_head.T, r_head.T

        r_full = []
        for layer in range(layers):
            att = lax.all_gather(jnp.concatenate([r_q[layer], r_kv[layer]], axis=1), both, axis=0, tiled=True)
            r_full.append([att] + [lax.all_gather(w[layer], both, axis=0, tiled=True) for w in (r_o, r_gu, r_dn)])

        chip_tok = tok_all[jnp.bitwise_xor(me, jnp.arange(2))]
        h = embed_rows(p_embed, chip_tok, core, 2, 640, [None, swap], 'fsdp', tok_all)

        def policy_layer(h, layer):
            h = attention_block(h, p_gains[2 * layer], tabs, p_qkv, p_wo, layer, core_arr)
            return mlp_block(h, p_gains[2 * layer + 1], p_gains[2 * layers], p_wgu, p_wdn, layer, layer == layers - 1, core_arr)

        def ref_layer(h, layer):
            w_qkv, w_o, w_gu, w_dn = r_full[layer]
            h = attention_block(h, r_gains[2 * layer], tabs, [w_qkv], [w_o], None, core_arr)
            return mlp_block(h, r_gains[2 * layer + 1], r_gains[2 * layers], [w_gu], [w_dn], None, layer == layers - 1, core_arr)

        h = policy_layer(h, 0)
        order, h = lax.optimization_barrier((tok_all[jnp.bitwise_xor(me, jnp.arange(n_dev))], h))
        h_ref = embed_rows(r_embed, order, me, n_dev, 192, xors, both, tok_all)
        h, h_ref = lax.optimization_barrier((h, h_ref))
        x = policy_layer(h, 1)
        x_peer = lax.ppermute(x, 'fsdp', swap)
        tgt_own = tgt_all[me] - core * p_head.shape[1]
        tgt_peer = tgt_all[jnp.bitwise_xor(me, 1)] - core * p_head.shape[1]

        h_ref, x = lax.optimization_barrier((h_ref, x))
        h_ref = ref_layer(h_ref, 0)
        x, h_ref = lax.optimization_barrier((x, h_ref))
        own = head_block(x, p_head, tgt_own)
        h_ref, own = lax.optimization_barrier((h_ref, own))
        x_ref = ref_layer(h_ref, 1)
        x_peer, x_ref = lax.optimization_barrier((x_peer, x_ref))
        x_all = [lax.all_gather(x_ref[at:at + t // 2], both, axis=0, tiled=True) for at in (0, t // 2)]
        peer = head_block(x_peer, p_head, tgt_peer)

        x_all[0], peer = lax.optimization_barrier((x_all[0], peer))
        parts = [jnp.stack(own + peer)]
        for half in range(2):
            tgt = tgt_all[:, half * (t // 2):(half + 1) * (t // 2)].reshape(-1) - me * r_head.shape[1]
            parts += [out.reshape(n_dev // 2, t) for out in head_block(x_all[half], r_head, tgt)]
        parts = lax.all_gather(jnp.concatenate(parts, axis=0), both)
        p_part = parts[:, :4]
        r_part = parts[:, 4:].reshape(n_dev, 2, 2, n_dev, t // 2)
        r_part = jnp.transpose(r_part, (2, 0, 3, 1, 4)).reshape(2, n_dev, n_dev, t)

        def finish(lse, picked):
            next_lp = (jnp.sum(picked, axis=0) - jax.nn.logsumexp(lse, axis=0)).reshape(n_dev * rows, SEQ)
            return jnp.where(jnp.arange(SEQ)[None, :] == 0, 0.0, jnp.roll(next_lp, 1, axis=1))

        logp_ref = finish(r_part[0], r_part[1])
        by_peer = p_part.reshape(n_dev // 2, 2, 4, t)[:, ::-1].reshape(n_dev, 4, t)
        lse = jnp.stack([p_part[:, 0], by_peer[:, 2]])
        picked = jnp.stack([p_part[:, 1], by_peer[:, 3]])
        logp = finish(lse, picked)
        row_part = row_losses(logp, logp_ref, old_all, mask_all, advantages(reward_all, group_all))
        loss = jnp.sum(row_part) / row_part.shape[0]
        return loss, lax.dynamic_slice_in_dim(logp, me * rows, rows), lax.dynamic_slice_in_dim(logp_ref, me * rows, rows)

    return jax.shard_map(device_step, mesh=mesh, in_specs=in_specs, out_specs=out_specs, check_vma=False)
```

```python
import functools

import jax
import jax.numpy as jnp
from jax import lax
from jax.experimental import pallas as pl
from jax.experimental.pallas import tpu as pltpu
from jax.sharding import PartitionSpec as P


HEAD_DIM = 64
EPS = 1e-6
ROPE_BASE = 10000.0
CLIP_EPS = 0.2
BETA = 0.04
ADV_EPS = 1e-4

F32 = jnp.float32
BF16 = jnp.bfloat16
NEG = -3.0e38
VMEM_LIMIT = 62 * 1024 * 1024

D = 1600
QH = 25
KVH = 5
QKV = 2240
O_AT = 2304
FF = 4352
SEQ = 32
TB = 256
SUB = 128
FT = 256
VT = 2048
HT = 512


def dot(lhs, rhs):
    return lax.dot_general(lhs, rhs, (((1,), (0,)), ((), ())), preferred_element_type=F32)


def dot_nt(lhs, rhs):
    return lax.dot_general(lhs, rhs, (((1,), (1,)), ((), ())), preferred_element_type=F32)


def rms(x, gain):
    x = x.astype(F32)
    inv = lax.rsqrt(jnp.sum(x * x, axis=-1, keepdims=True) * (1.0 / D) + EPS)
    return (x * inv * gain).astype(BF16)


def row_copies(parts, layer, half_of, dst, sems, base):
    out = []
    for p, part in enumerate(parts):
        src = part if layer is None else part.at[layer]
        rows = src.shape[0]
        at = pl.multiple_of(half_of(p) * rows, 8) if len(parts) > 1 else 0
        out.append(pltpu.make_async_copy(src, dst.at[pl.ds(at, rows)], sems.at[base + p]))
    return out


def attn_kernel(n, layer, core_ref, h_ref, gain_ref, cos_ref, sin_ref, *refs):
    out_ref, w_s, qkv_s, qk_s, o_s, sc_s, p_s, sems = refs[n:]
    core = core_ref[0]

    def half_of(p):
        return jnp.bitwise_xor(core, p)

    copies = row_copies(refs[:n], layer, half_of, w_s, sems, 0)
    for copy in copies:
        copy.start()
    for copy in copies:
        copy.wait()

    lane = lax.broadcasted_iota(jnp.int32, (1, 128), 1)
    low_half = lane < 64
    rot_mask = (lane % 64) < 32
    q_idx = lax.broadcasted_iota(jnp.int32, (SUB, 2 * SUB), 0)
    k_idx = lax.broadcasted_iota(jnp.int32, (SUB, 2 * SUB), 1) % SUB
    keep = (q_idx // SEQ == k_idx // SEQ) & (k_idx <= q_idx)
    zero = jnp.zeros((), BF16)

    def project(b):
        rows = pl.ds(pl.multiple_of(b * TB, TB), TB)
        qkv_s[...] = dot(rms(h_ref[rows, :], gain_ref[...]), w_s[:, :QKV])
        cos, sin = cos_ref[...], sin_ref[...]
        for j in range(15):
            x = qkv_s[:, 128 * j:128 * (j + 1)]
            rot = jnp.where(rot_mask, pltpu.roll(x, 96, 1), pltpu.roll(x, 32, 1))
            qk_s[:, 128 * j:128 * (j + 1)] = (x * cos + rot * sin).astype(BF16)

    def attend(s):
        rows = slice(s * SUB, (s + 1) * SUB)
        k_pads, v_pads = [], []
        for g in range(KVH):
            c, side = divmod(25 + g, 2)
            x = qk_s[rows, 128 * c:128 * (c + 1)].astype(F32)
            y = pltpu.roll(x, 64, 1)
            at_low, at_high = (y, x) if side else (x, y)
            k_pads.append((jnp.where(low_half, at_low, 0.0).astype(BF16), jnp.where(low_half, 0.0, at_high).astype(BF16)))
            c, side = divmod(g, 2)
            if c < 2:
                x = qkv_s[rows, 1920 + 128 * c:2048 + 128 * c]
            else:
                x = jnp.concatenate([qkv_s[rows, 2176:2240], jnp.zeros((SUB, 64), F32)], axis=1)
            y = pltpu.roll(x, 64, 1)
            at_low, at_high = (y, x) if side else (x, y)
            v_pads.append((jnp.where(low_half, at_low, 0.0).astype(BF16), jnp.where(low_half, 0.0, at_high).astype(BF16)))
        heads = [((2 * j) // 5, min((2 * j + 1) // 5, KVH - 1)) for j in range(13)]
        for j, (ga, gb) in enumerate(heads):
            keys = jnp.concatenate([k_pads[ga][0], k_pads[gb][1]], axis=0)
            scores = dot_nt(qk_s[rows, 128 * j:128 * (j + 1)], keys) * (HEAD_DIM ** -0.5)
            sc_s[:, 2 * SUB * j:2 * SUB * (j + 1)] = jnp.where(keep, scores, -1e30)
        for i in range(QH):
            x = sc_s[:, SUB * i:SUB * (i + 1)]
            e = jnp.exp(x - jnp.max(x, axis=1, keepdims=True))
            p_s[:, SUB * i:SUB * (i + 1)] = (e * (1.0 / jnp.sum(e, axis=1, keepdims=True))).astype(BF16)
        for j, (ga, gb) in enumerate(heads):
            if j < 12:
                vals = jnp.concatenate([v_pads[ga][0], v_pads[gb][1]], axis=0)
                o_s[rows, 128 * j:128 * (j + 1)] = dot(p_s[:, 2 * SUB * j:2 * SUB * (j + 1)], vals).astype(BF16)
            else:
                o_s[rows, 1536:1600] = dot(p_s[:, 2 * SUB * j:2 * SUB * j + SUB], v_pads[ga][0]).astype(BF16)[:, :64]

    def block(b, carry):
        rows = pl.ds(pl.multiple_of(b * TB, TB), TB)
        project(b)
        for s in range(TB // SUB):
            attend(s)
        out_ref[rows, :] = (h_ref[rows, :].astype(F32) + dot(o_s[...], w_s[:, O_AT:])).astype(BF16)
        return carry

    lax.fori_loop(0, h_ref.shape[0] // TB, block, 0)


def attention_block(h, gain, tabs, w_att, layer, core):
    n = len(w_att)
    t = h.shape[0]
    vm = pl.BlockSpec(memory_space=pltpu.VMEM)
    anym = pl.BlockSpec(memory_space=pl.ANY)
    return pl.pallas_call(
        functools.partial(attn_kernel, n, layer),
        out_shape=jax.ShapeDtypeStruct((t, D), BF16),
        in_specs=[pl.BlockSpec(memory_space=pltpu.SMEM), vm, vm, vm, vm] + [anym] * n,
        out_specs=vm,
        scratch_shapes=[
            pltpu.VMEM((D, O_AT + D), BF16), pltpu.VMEM((TB, QKV), F32),
            pltpu.VMEM((TB, 1920), BF16), pltpu.VMEM((TB, D), BF16), pltpu.VMEM((SUB, 26 * SUB), F32), pltpu.VMEM((SUB, 26 * SUB), BF16),
            pltpu.SemaphoreType.DMA((n,)),
        ],
        compiler_params=pltpu.CompilerParams(vmem_limit_bytes=VMEM_LIMIT),
        cost_estimate=pl.CostEstimate(flops=2 * t * D * (QKV + D), bytes_accessed=2 * D * (QKV + D), transcendentals=0),
        name="attn",
    )(core, h, gain, tabs[0], tabs[1], *w_att)


def mlp_kernel(n, layer, last, core_ref, h_ref, gain_ref, fin_ref, *refs):
    gu_parts, dn_parts = refs[:n], refs[n:2 * n]
    out_ref, wg, wu, wd, c_s, act_s, acc, sems, dn_sems = refs[2 * n:]
    core = core_ref[0]
    steps = FF // FT
    half_subs = FF // 2 // 128

    def gu_copies(j, slot):
        out = []
        for p, part in enumerate(gu_parts):
            src = part if layer is None else part.at[layer]
            rows = src.shape[0]
            at = pl.multiple_of(jnp.bitwise_xor(core, p) * rows, 8) if n > 1 else 0
            for t, dst in enumerate((wg, wu)):
                cols = pl.ds(pl.multiple_of(t * FF + j * FT, 128), FT)
                out.append(pltpu.make_async_copy(src.at[:, cols], dst.at[slot, pl.ds(at, rows)], sems.at[slot, 2 * p + t]))
        return out

    def dn_copy(part, j, i):
        slot = lax.rem(j, 3)
        src = part if layer is None else part.at[layer]
        if n == 1:
            at = pl.multiple_of(j * FT, FT)
            return pltpu.make_async_copy(src.at[pl.ds(at, FT)], wd.at[slot], dn_sems.at[slot, 0])
        sub = 2 * j + i
        col = pl.multiple_of(jnp.where(sub >= half_subs, sub - half_subs, sub) * 128, 128)
        return pltpu.make_async_copy(src.at[:, pl.ds(col, 128)], wd.at[slot, :, pl.ds(128 * i, 128)], dn_sems.at[slot, i])

    def start(j):
        for copy in gu_copies(j, lax.rem(j, 2)):
            copy.start()
        if n == 1:
            dn_copy(dn_parts[0], j, 0).start()
        else:
            for i in range(2):
                half = (2 * j + i >= half_subs).astype(jnp.int32)
                mine = half == core

                @pl.when(mine)
                def _():
                    dn_copy(dn_parts[0], j, i).start()

                @pl.when(jnp.logical_not(mine))
                def _():
                    dn_copy(dn_parts[1], j, i).start()

    def wait_gu(j):
        for copy in gu_copies(j, lax.rem(j, 2)):
            copy.wait()

    def wait_dn(j):
        for i in range(n):
            dn_copy(dn_parts[0], j, i).wait()

    def gate_up(j):
        slot = lax.rem(j, 2)
        g = dot(c_s[...], wg[slot])
        u = dot(c_s[...], wu[slot])
        act_s[slot] = (g * jax.nn.sigmoid(g) * u).astype(BF16)

    def down(j):
        act, w = act_s[lax.rem(j, 2)], wd[lax.rem(j, 3)]
        acc[...] += dot(act, w) if n == 1 else dot_nt(act, w)

    zero = jnp.int32(0)
    start(zero)
    start(zero + 1)
    c_s[...] = rms(h_ref[...], gain_ref[...])
    acc[...] = h_ref[...].astype(F32)
    wait_gu(zero)
    gate_up(zero)

    def step(j, carry):
        @pl.when(j + 1 < steps)
        def _():
            start(j + 1)

        wait_gu(j)
        wait_dn(j - 1)
        gate_up(j)
        down(j - 1)
        return carry

    lax.fori_loop(1, steps, step, 0)
    wait_dn(zero + (steps - 1))
    down(zero + (steps - 1))
    out = acc[...].astype(BF16)
    out_ref[...] = rms(out, fin_ref[...]) if last else out


def mlp_block(h, gain, fin, w_gu, w_dn, layer, last, core):
    n = len(w_gu)
    t = h.shape[0]
    vm = pl.BlockSpec(memory_space=pltpu.VMEM)
    anym = pl.BlockSpec(memory_space=pl.ANY)
    return pl.pallas_call(
        functools.partial(mlp_kernel, n, layer, last),
        out_shape=jax.ShapeDtypeStruct((t, D), BF16),
        in_specs=[pl.BlockSpec(memory_space=pltpu.SMEM), vm, vm, vm] + [anym] * (2 * n),
        out_specs=vm,
        scratch_shapes=[
            pltpu.VMEM((2, D, FT), BF16), pltpu.VMEM((2, D, FT), BF16), pltpu.VMEM((3, FT, D) if n == 1 else (3, D, FT), BF16),
            pltpu.VMEM((t, D), BF16), pltpu.VMEM((2, t, FT), BF16), pltpu.VMEM((t, D), F32),
            pltpu.SemaphoreType.DMA((2, 4)), pltpu.SemaphoreType.DMA((3, 2)),
        ],
        compiler_params=pltpu.CompilerParams(vmem_limit_bytes=VMEM_LIMIT),
        cost_estimate=pl.CostEstimate(flops=6 * t * D * FF, bytes_accessed=6 * D * FF, transcendentals=0),
        name="mlp",
    )(core, h, gain, fin, *w_gu, *w_dn)


def gate_up_kernel(h_ref, gain_ref, wg_ref, wu_ref, act_ref, c_s):
    @pl.when(pl.program_id(0) == 0)
    def _():
        c_s[...] = rms(h_ref[...], gain_ref[...])

    g = dot(c_s[...], wg_ref[...])
    u = dot(c_s[...], wu_ref[...])
    act_ref[...] = (g * jax.nn.sigmoid(g) * u).astype(BF16)


def down_kernel(h_ref, act_ref, w_ref, fin_ref, out_ref, acc):
    j = pl.program_id(0)

    @pl.when(j == 0)
    def _():
        acc[...] = h_ref[...].astype(F32)

    acc[...] += dot(act_ref[...], w_ref[...])

    @pl.when(j == pl.num_programs(0) - 1)
    def _():
        out_ref[...] = rms(acc[...].astype(BF16), fin_ref[...])


def gate_up(h, gain, w_gu):
    t, steps = h.shape[0], FF // FT
    fixed = lambda j: (0, 0)
    return pl.pallas_call(
        gate_up_kernel,
        out_shape=jax.ShapeDtypeStruct((t, FF), BF16),
        grid=(steps,),
        in_specs=[
            pl.BlockSpec((t, D), fixed), pl.BlockSpec((1, D), fixed),
            pl.BlockSpec((D, FT), lambda j: (0, j)), pl.BlockSpec((D, FT), lambda j: (0, steps + j)),
        ],
        out_specs=pl.BlockSpec((t, FT), lambda j: (0, j)),
        scratch_shapes=[pltpu.VMEM((t, D), BF16)],
        compiler_params=pltpu.CompilerParams(vmem_limit_bytes=VMEM_LIMIT),
        cost_estimate=pl.CostEstimate(flops=4 * t * D * FF, bytes_accessed=4 * D * FF, transcendentals=0),
        name="gate_up",
    )(h, gain, w_gu, w_gu)


def down_norm(h, act, w_dn, fin):
    t = h.shape[0]
    fixed = lambda j: (0, 0)
    return pl.pallas_call(
        down_kernel,
        out_shape=jax.ShapeDtypeStruct((t, D), BF16),
        grid=(FF // FT,),
        in_specs=[
            pl.BlockSpec((t, D), fixed), pl.BlockSpec((t, FT), lambda j: (0, j)),
            pl.BlockSpec((FT, D), lambda j: (j, 0)), pl.BlockSpec((1, D), fixed),
        ],
        out_specs=pl.BlockSpec((t, D), fixed),
        scratch_shapes=[pltpu.VMEM((t, D), F32)],
        compiler_params=pltpu.CompilerParams(vmem_limit_bytes=VMEM_LIMIT),
        cost_estimate=pl.CostEstimate(flops=2 * t * D * FF, bytes_accessed=2 * D * FF, transcendentals=0),
        name="down",
    )(h, act, w_dn, fin)


def head_kernel(vocab, x_ref, w_ref, tgt_ref, out_ref, lg_s, m_s, s_s, p_s):
    j = pl.program_id(1)

    @pl.when(j == 0)
    def _():
        m_s[...] = jnp.full(m_s.shape, NEG, F32)
        s_s[...] = jnp.zeros(s_s.shape, F32)
        p_s[...] = jnp.zeros(p_s.shape, F32)

    lane = lax.broadcasted_iota(jnp.int32, m_s.shape, 1)
    rel = tgt_ref[...] - lane - j * VT
    held = vocab - j * VT

    def update(k):
        at = k * HT
        cols = [lg_s[k % 2, :, 128 * c:128 * (c + 1)] for c in range(HT // 128)]
        if at + HT > (vocab % VT or VT):
            cols = [jnp.where(lane < held - at - 128 * c, x, NEG) for c, x in enumerate(cols)]
        m_old = m_s[...]
        m_new = functools.reduce(jnp.maximum, cols, m_old)
        s_s[...] = s_s[...] * jnp.exp(m_old - m_new) + sum(jnp.exp(x - m_new) for x in cols)
        m_s[...] = m_new
        picked = 0.0
        for c, x in enumerate(cols):
            picked = jnp.where(rel == at + 128 * c, x, picked)
        p_s[...] += picked

    for k in range(VT // HT):
        lg_s[k % 2] = dot(x_ref[...], w_ref[:, k * HT:(k + 1) * HT])
        if k:
            update(k - 1)
    update(VT // HT - 1)

    @pl.when(j == pl.num_programs(1) - 1)
    def _():
        m = m_s[...]
        top = jnp.max(m, axis=1, keepdims=True)
        lse = top + jnp.log(jnp.sum(s_s[...] * jnp.exp(m - top), axis=1, keepdims=True))
        picked = jnp.sum(p_s[...], axis=1, keepdims=True)
        out_ref[...] = jnp.where(lane == 0, lse, picked)


def head_block(x, w, tgt, tt=1024):
    t, v = x.shape[0], w.shape[1]
    tgt = jnp.broadcast_to(jnp.where((tgt >= 0) & (tgt < v), tgt, -1)[:, None], (t, 128))
    out = pl.pallas_call(
        functools.partial(head_kernel, v),
        out_shape=jax.ShapeDtypeStruct((t, 128), F32),
        grid=(t // tt, pl.cdiv(v, VT)),
        in_specs=[
            pl.BlockSpec((tt, D), lambda i, j: (i, 0)), pl.BlockSpec((D, VT), lambda i, j: (0, j)),
            pl.BlockSpec((tt, 128), lambda i, j: (i, 0)),
        ],
        out_specs=pl.BlockSpec((tt, 128), lambda i, j: (i, 0)),
        scratch_shapes=[pltpu.VMEM((2, tt, HT), F32)] + [pltpu.VMEM((tt, 128), F32)] * 3,
        compiler_params=pltpu.CompilerParams(vmem_limit_bytes=VMEM_LIMIT),
        cost_estimate=pl.CostEstimate(flops=2 * t * D * v, bytes_accessed=2 * D * (v * t // tt + t), transcendentals=t * v),
        name="head",
    )(x, w, tgt)
    return out[:, 0], out[:, 1]


def rope_tables():
    half = HEAD_DIM // 2
    inv_freq = ROPE_BASE ** (-jnp.arange(half, dtype=F32) / half)
    angles = jnp.arange(SEQ, dtype=F32)[:, None] * inv_freq[None, :]
    cos, sin = jnp.cos(angles), jnp.sin(angles)
    cos = jnp.tile(jnp.concatenate([cos, cos] * 2, axis=1), (TB // SEQ, 1))
    sin = jnp.tile(jnp.concatenate([-sin, sin] * 2, axis=1), (TB // SEQ, 1))
    return cos, sin


def running_count(flags):
    n = flags.shape[-1]
    upper = (jnp.arange(n)[:, None] <= jnp.arange(n)[None, :]).astype(BF16)
    return dot(flags.astype(BF16), upper).astype(jnp.int32)


def embed_send(table, toks, me, cap, r):
    size, vocab = toks.shape[0], table.shape[0]
    local = toks - me * vocab
    owned = (local >= 0) & (local < vocab)
    rank = running_count(owned) - 1
    slots = r * cap + jnp.arange(cap)
    hit = owned[:, None, :] & (rank[:, None, :] == slots[None, :, None])
    idx = jnp.sum(jnp.where(hit, local[:, None, :], 0), axis=2)
    rows = jnp.take(table, idx.reshape(-1), axis=0).reshape(size, cap, D)
    return [rows[k] for k in range(size)]


def embed_swap(rows, perms, axis):
    return rows[:1] + [lax.ppermute(rows[k], axis, perms[k]) for k in range(1, len(rows))]


def embed_pick(got, tok, vocab, me, cap, r):
    size, t = len(got), tok.shape[0]
    peers = jnp.bitwise_xor(me, jnp.arange(size))
    wanted = (tok // vocab)[None, :] == peers[:, None]
    slot = running_count(wanted) - 1 - r * cap
    pick = wanted[:, :, None] & (slot[:, :, None] == jnp.arange(cap)[None, None, :])
    pick = jnp.swapaxes(pick, 0, 1).reshape(t, size * cap).astype(BF16)
    return dot(pick, jnp.concatenate(got, axis=0)).astype(BF16)


def advantages(rewards, groups):
    same = (groups[:, None] == groups[None, :]).astype(F32)
    counts = jnp.sum(same, axis=1)
    means = jnp.sum(same * rewards[None, :], axis=1) / counts
    centred = rewards - means
    spread = jnp.sqrt(jnp.sum(same * (centred * centred)[None, :], axis=1) / counts)
    return centred / (spread + ADV_EPS)


def row_losses(logp, logp_ref, logp_old, weights, advantage):
    log_gap = logp_ref - logp
    kl_est = jnp.exp(log_gap) - log_gap - 1.0
    ratio = jnp.exp(logp - logp_old)
    adv_row = advantage[:, None]
    surrogate = jnp.minimum(ratio * adv_row, jnp.clip(ratio, 1.0 - CLIP_EPS, 1.0 + CLIP_EPS) * adv_row)
    per_token = -surrogate + BETA * kl_est
    return jnp.sum(per_token * weights, axis=1) / jnp.sum(weights, axis=1)


def solution(mesh):
    both = ('rep', 'fsdp')
    row_spec = P(both, None)
    n_dev = mesh.shape['rep'] * mesh.shape['fsdp']
    swap = [(0, 1), (1, 0)]
    xors = [[(d, d ^ k) for d in range(n_dev)] for k in range(n_dev)]

    def weight_specs(axes):
        return [P(None, axes, None)] * 5 + [P(None, axes), P(axes, None), P(axes, None)]

    in_specs = tuple([row_spec, row_spec, row_spec, P(both), P(both)] + weight_specs('fsdp') + weight_specs(both))
    out_specs = (P(), row_spec, row_spec)

    def device_step(tokens, resp_mask, logp_old, rewards, group_id, *weights):
        p_q, p_kv, p_o, p_gu, p_dn, p_norms, p_embed, p_head = weights[:8]
        r_q, r_kv, r_o, r_gu, r_dn, r_norms, r_embed, r_head = weights[8:]
        core = lax.axis_index('fsdp')
        me = lax.axis_index('rep') * 2 + core
        core_arr = core.astype(jnp.int32).reshape(1)
        rows = tokens.shape[0]
        t = rows * SEQ
        layers = p_q.shape[0]
        tabs = rope_tables()

        tok = tokens.reshape(t)
        tok_pair = jnp.stack([tok, lax.ppermute(tok, 'fsdp', swap)])
        local = tok_pair - core * p_embed.shape[0]
        looked = jnp.take(p_embed, jnp.clip(local, 0, p_embed.shape[0] - 1), axis=0)
        from_peer = lax.ppermute(looked[1], 'fsdp', swap)
        h = jnp.where(((local[0] >= 0) & (local[0] < p_embed.shape[0]))[:, None], looked[0], from_peer)
        p_gains = jnp.stack([p_norms, lax.ppermute(p_norms, 'fsdp', swap)]).astype(F32)
        p_gains = jnp.where(core == 0, p_gains, p_gains[::-1])
        p_gains = jnp.swapaxes(p_gains, 0, 1).reshape(2 * layers + 1, 1, D)

        smalls = (tokens, resp_mask, logp_old, rewards, group_id, r_norms)
        small = jnp.concatenate([x.astype(F32).reshape(-1) for x in smalls])
        small = jnp.pad(small, (0, -small.size % 1024)).reshape(-1, 128)
        small = jnp.stack([small] + [lax.ppermute(small, both, xors[k]) for k in range(1, n_dev)])
        xor_ids = jnp.bitwise_xor(me, jnp.arange(n_dev))
        order = small.reshape(n_dev, -1)[:, :t].astype(jnp.int32)
        small = small[xor_ids].reshape(n_dev, -1)
        cuts, at = [], 0
        for x in smalls:
            cuts.append(small[:, at:at + x.size].reshape((n_dev,) + x.shape))
            at += x.size
        tok_all = cuts[0].astype(jnp.int32).reshape(n_dev, t)
        mask_all, old_all = (x.reshape(n_dev * rows, SEQ) for x in cuts[1:3])
        reward_all = cuts[3].reshape(-1)
        group_all = cuts[4].reshape(-1)
        r_gains = jnp.swapaxes(cuts[5], 0, 1).reshape(2 * layers + 1, 1, D)
        tgt_all = jnp.roll(tok_all.reshape(n_dev * rows, SEQ), -1, axis=1).reshape(n_dev, t)

        def attention_weights(q, kv, o):
            return jnp.concatenate([q, kv, jnp.zeros(q.shape[:-1] + (O_AT - QKV,), BF16), o], axis=-1)

        p_att = attention_weights(p_q, p_kv, p_o)
        p_parts = []
        for w in (p_att, p_gu, jnp.swapaxes(p_dn, 1, 2)):
            p_parts.append([w, lax.ppermute(w, 'fsdp', swap)])
        p_att, p_wgu, p_wdn = p_parts
        p_head, r_head = p_head.T, r_head.T

        def ref_weights(layer, dn):
            att = attention_weights(r_q[layer], r_kv[layer], r_o[layer])
            return [lax.all_gather(w, both, axis=0, tiled=True) for w in (att, r_gu[layer], dn)]

        def policy_layer(h, layer):
            h = attention_block(h, p_gains[2 * layer], tabs, p_att, layer, core_arr)
            return mlp_block(h, p_gains[2 * layer + 1], p_gains[2 * layers], p_wgu, p_wdn, layer, layer == layers - 1, core_arr)

        r_full = [ref_weights(0, r_dn[0])]
        h = policy_layer(h, 0)
        order, dn, h = lax.optimization_barrier((order, r_dn[1], h))
        r_full.append(ref_weights(1, dn))
        cap = 192
        h, got = lax.optimization_barrier((h, embed_send(r_embed, order, me, cap, 0)))
        got = embed_swap(got, xors, both)
        x = policy_layer(h, 1)
        x_peer = lax.ppermute(x, 'fsdp', swap)
        got, x = lax.optimization_barrier((got, x))
        h_ref = embed_pick(got, tok, r_embed.shape[0], me, cap, 0)
        counts = jnp.sum((tok_all[:, None, :] // r_embed.shape[0]) == jnp.arange(n_dev)[None, :, None], axis=2)
        h_ref = lax.fori_loop(1, (jnp.max(counts) + cap - 1) // cap, lambda r, acc: acc + embed_pick(
            embed_swap(embed_send(r_embed, order, me, cap, r), xors, both), tok, r_embed.shape[0], me, cap, r), h_ref)
        tgt_own = tgt_all[me] - core * p_head.shape[1]
        tgt_peer = tgt_all[jnp.bitwise_xor(me, 1)] - core * p_head.shape[1]

        h_ref, x = lax.optimization_barrier((h_ref, x))
        att, w_gu, w_dn = r_full[0]
        h_ref = attention_block(h_ref, r_gains[0], tabs, [att], None, core_arr)
        h_ref = mlp_block(h_ref, r_gains[1], r_gains[2 * layers], [w_gu], [w_dn], None, False, core_arr)
        x, h_ref = lax.optimization_barrier((x, h_ref))
        own = head_block(x, p_head, tgt_own)
        h_ref, own = lax.optimization_barrier((h_ref, own))
        att, w_gu, w_dn = r_full[1]
        h_ref = attention_block(h_ref, r_gains[2], tabs, [att], None, core_arr)
        act = gate_up(h_ref, r_gains[3], w_gu)
        x_ref = down_norm(h_ref, act, w_dn, r_gains[2 * layers])
        x_peer, x_ref = lax.optimization_barrier((x_peer, x_ref))
        x_all = [lax.all_gather(x_ref[at:at + t // 2], both, axis=0, tiled=True) for at in (0, t // 2)]
        peer = head_block(x_peer, p_head, tgt_peer)

        x_all[0], peer = lax.optimization_barrier((x_all[0], peer))
        parts = [jnp.stack(own + peer)]
        for half in range(2):
            tgt = tgt_all[:, half * (t // 2):(half + 1) * (t // 2)].reshape(-1) - me * r_head.shape[1]
            parts += [out.reshape(n_dev // 2, t) for out in head_block(x_all[half], r_head, tgt)]
        parts = lax.all_gather(jnp.concatenate(parts, axis=0), both)
        p_part = parts[:, :4]
        r_part = parts[:, 4:].reshape(n_dev, 2, 2, n_dev, t // 2)
        r_part = jnp.transpose(r_part, (2, 0, 3, 1, 4)).reshape(2, n_dev, n_dev, t)

        def finish(lse, picked):
            next_lp = (jnp.sum(picked, axis=0) - jax.nn.logsumexp(lse, axis=0)).reshape(n_dev * rows, SEQ)
            return jnp.where(jnp.arange(SEQ)[None, :] == 0, 0.0, jnp.roll(next_lp, 1, axis=1))

        logp_ref = finish(r_part[0], r_part[1])
        by_peer = p_part.reshape(n_dev // 2, 2, 4, t)[:, ::-1].reshape(n_dev, 4, t)
        lse = jnp.stack([p_part[:, 0], by_peer[:, 2]])
        picked = jnp.stack([p_part[:, 1], by_peer[:, 3]])
        logp = finish(lse, picked)
        row_part = row_losses(logp, logp_ref, old_all, mask_all, advantages(reward_all, group_all))
        loss = jnp.sum(row_part) / row_part.shape[0]
        return loss, lax.dynamic_slice_in_dim(logp, me * rows, rows), lax.dynamic_slice_in_dim(logp_ref, me * rows, rows)

    return jax.shard_map(device_step, mesh=mesh, in_specs=in_specs, out_specs=out_specs, check_vma=False)
```

```python
import functools

import jax
import jax.numpy as jnp
from jax import lax
from jax.experimental import pallas as pl
from jax.experimental.pallas import tpu as pltpu
from jax.sharding import PartitionSpec as P


HEAD_DIM = 64
EPS = 1e-6
ROPE_BASE = 10000.0
CLIP_EPS = 0.2
BETA = 0.04
ADV_EPS = 1e-4

F32 = jnp.float32
BF16 = jnp.bfloat16
NEG = -3.0e38
VMEM_LIMIT = 62 * 1024 * 1024

D = 1600
QH = 25
KVH = 5
QKV = 2240
O_AT = 2304
FF = 4352
SEQ = 32
TB = 256
SUB = 128
FT = 256
RT = 640
VT = 2048
HT = 512


def dot(lhs, rhs):
    return lax.dot_general(lhs, rhs, (((1,), (0,)), ((), ())), preferred_element_type=F32)


def dot_nt(lhs, rhs):
    return lax.dot_general(lhs, rhs, (((1,), (1,)), ((), ())), preferred_element_type=F32)


def rms(x, gain):
    x = x.astype(F32)
    inv = lax.rsqrt(jnp.sum(x * x, axis=-1, keepdims=True) * (1.0 / D) + EPS)
    return (x * inv * gain).astype(BF16)


def row_copies(parts, layer, half_of, dst, sems, base):
    out = []
    for p, part in enumerate(parts):
        src = part if layer is None else part.at[layer]
        rows = src.shape[0]
        at = pl.multiple_of(half_of(p) * rows, 8) if len(parts) > 1 else 0
        out.append(pltpu.make_async_copy(src, dst.at[pl.ds(at, rows)], sems.at[base + p]))
    return out


def attn_kernel(n, layer, core_ref, h_ref, gain_ref, cos_ref, sin_ref, *refs):
    out_ref, w_s, qkv_s, qk_s, o_s, sc_s, p_s, sems = refs[n:]
    core = core_ref[0]

    def half_of(p):
        return jnp.bitwise_xor(core, p)

    copies = row_copies(refs[:n], layer, half_of, w_s, sems, 0)
    for copy in copies:
        copy.start()
    for copy in copies:
        copy.wait()

    lane = lax.broadcasted_iota(jnp.int32, (1, 128), 1)
    low_half = lane < 64
    rot_mask = (lane % 64) < 32
    q_idx = lax.broadcasted_iota(jnp.int32, (SUB, 2 * SUB), 0)
    k_idx = lax.broadcasted_iota(jnp.int32, (SUB, 2 * SUB), 1) % SUB
    keep = (q_idx // SEQ == k_idx // SEQ) & (k_idx <= q_idx)
    zero = jnp.zeros((), BF16)

    def project(b):
        rows = pl.ds(pl.multiple_of(b * TB, TB), TB)
        qkv_s[...] = dot(rms(h_ref[rows, :], gain_ref[...]), w_s[:, :QKV])
        cos, sin = cos_ref[...], sin_ref[...]
        for j in range(15):
            x = qkv_s[:, 128 * j:128 * (j + 1)]
            rot = jnp.where(rot_mask, pltpu.roll(x, 96, 1), pltpu.roll(x, 32, 1))
            qk_s[:, 128 * j:128 * (j + 1)] = (x * cos + rot * sin).astype(BF16)

    def attend(s):
        rows = slice(s * SUB, (s + 1) * SUB)
        k_pads, v_pads = [], []
        for g in range(KVH):
            c, side = divmod(25 + g, 2)
            x = qk_s[rows, 128 * c:128 * (c + 1)].astype(F32)
            y = pltpu.roll(x, 64, 1)
            at_low, at_high = (y, x) if side else (x, y)
            k_pads.append((jnp.where(low_half, at_low, 0.0).astype(BF16), jnp.where(low_half, 0.0, at_high).astype(BF16)))
            c, side = divmod(g, 2)
            if c < 2:
                x = qkv_s[rows, 1920 + 128 * c:2048 + 128 * c]
            else:
                x = jnp.concatenate([qkv_s[rows, 2176:2240], jnp.zeros((SUB, 64), F32)], axis=1)
            y = pltpu.roll(x, 64, 1)
            at_low, at_high = (y, x) if side else (x, y)
            v_pads.append((jnp.where(low_half, at_low, 0.0).astype(BF16), jnp.where(low_half, 0.0, at_high).astype(BF16)))
        heads = [((2 * j) // 5, min((2 * j + 1) // 5, KVH - 1)) for j in range(13)]
        for j, (ga, gb) in enumerate(heads):
            keys = jnp.concatenate([k_pads[ga][0], k_pads[gb][1]], axis=0)
            scores = dot_nt(qk_s[rows, 128 * j:128 * (j + 1)], keys) * (HEAD_DIM ** -0.5)
            sc_s[:, 2 * SUB * j:2 * SUB * (j + 1)] = jnp.where(keep, scores, -1e30)
        for i in range(QH):
            x = sc_s[:, SUB * i:SUB * (i + 1)]
            e = jnp.exp(x - jnp.max(x, axis=1, keepdims=True))
            p_s[:, SUB * i:SUB * (i + 1)] = (e * (1.0 / jnp.sum(e, axis=1, keepdims=True))).astype(BF16)
        for j, (ga, gb) in enumerate(heads):
            if j < 12:
                vals = jnp.concatenate([v_pads[ga][0], v_pads[gb][1]], axis=0)
                o_s[rows, 128 * j:128 * (j + 1)] = dot(p_s[:, 2 * SUB * j:2 * SUB * (j + 1)], vals).astype(BF16)
            else:
                o_s[rows, 1536:1600] = dot(p_s[:, 2 * SUB * j:2 * SUB * j + SUB], v_pads[ga][0]).astype(BF16)[:, :64]

    def block(b, carry):
        rows = pl.ds(pl.multiple_of(b * TB, TB), TB)
        project(b)
        for s in range(TB // SUB):
            attend(s)
        out_ref[rows, :] = (h_ref[rows, :].astype(F32) + dot(o_s[...], w_s[:, O_AT:])).astype(BF16)
        return carry

    lax.fori_loop(0, h_ref.shape[0] // TB, block, 0)


def attention_block(h, gain, tabs, w_att, layer, core):
    n = len(w_att)
    t = h.shape[0]
    vm = pl.BlockSpec(memory_space=pltpu.VMEM)
    anym = pl.BlockSpec(memory_space=pl.ANY)
    return pl.pallas_call(
        functools.partial(attn_kernel, n, layer),
        out_shape=jax.ShapeDtypeStruct((t, D), BF16),
        in_specs=[pl.BlockSpec(memory_space=pltpu.SMEM), vm, vm, vm, vm] + [anym] * n,
        out_specs=vm,
        scratch_shapes=[
            pltpu.VMEM((D, O_AT + D), BF16), pltpu.VMEM((TB, QKV), F32),
            pltpu.VMEM((TB, 1920), BF16), pltpu.VMEM((TB, D), BF16), pltpu.VMEM((SUB, 26 * SUB), F32), pltpu.VMEM((SUB, 26 * SUB), BF16),
            pltpu.SemaphoreType.DMA((n,)),
        ],
        compiler_params=pltpu.CompilerParams(vmem_limit_bytes=VMEM_LIMIT),
        cost_estimate=pl.CostEstimate(flops=2 * t * D * (QKV + D), bytes_accessed=2 * D * (QKV + D), transcendentals=0),
        name="attn",
    )(core, h, gain, tabs[0], tabs[1], *w_att)


def mlp_kernel(n, layer, last, core_ref, h_ref, gain_ref, fin_ref, *refs):
    gu_parts, dn_parts = refs[:n], refs[n:2 * n]
    out_ref, wg, wu, wd, c_s, act_s, acc, sems, dn_sems = refs[2 * n:]
    core = core_ref[0]
    steps = FF // FT
    half_subs = FF // 2 // 128

    def gu_copies(j, slot):
        out = []
        for p, part in enumerate(gu_parts):
            src = part if layer is None else part.at[layer]
            rows = src.shape[0]
            at = pl.multiple_of(jnp.bitwise_xor(core, p) * rows, 8) if n > 1 else 0
            for t, dst in enumerate((wg, wu)):
                cols = pl.ds(pl.multiple_of(t * FF + j * FT, 128), FT)
                out.append(pltpu.make_async_copy(src.at[:, cols], dst.at[slot, pl.ds(at, rows)], sems.at[slot, 2 * p + t]))
        return out

    def dn_copy(part, j, i):
        slot = lax.rem(j, 3)
        src = part if layer is None else part.at[layer]
        if n == 1:
            at = pl.multiple_of(j * FT, FT)
            return pltpu.make_async_copy(src.at[pl.ds(at, FT)], wd.at[slot], dn_sems.at[slot, 0])
        sub = 2 * j + i
        col = pl.multiple_of(jnp.where(sub >= half_subs, sub - half_subs, sub) * 128, 128)
        return pltpu.make_async_copy(src.at[:, pl.ds(col, 128)], wd.at[slot, :, pl.ds(128 * i, 128)], dn_sems.at[slot, i])

    def start(j):
        for copy in gu_copies(j, lax.rem(j, 2)):
            copy.start()
        if n == 1:
            dn_copy(dn_parts[0], j, 0).start()
        else:
            for i in range(2):
                half = (2 * j + i >= half_subs).astype(jnp.int32)
                mine = half == core

                @pl.when(mine)
                def _():
                    dn_copy(dn_parts[0], j, i).start()

                @pl.when(jnp.logical_not(mine))
                def _():
                    dn_copy(dn_parts[1], j, i).start()

    def wait_gu(j):
        for copy in gu_copies(j, lax.rem(j, 2)):
            copy.wait()

    def wait_dn(j):
        for i in range(n):
            dn_copy(dn_parts[0], j, i).wait()

    def gate_up(j):
        slot = lax.rem(j, 2)
        g = dot(c_s[...], wg[slot])
        u = dot(c_s[...], wu[slot])
        act_s[slot] = (g * jax.nn.sigmoid(g) * u).astype(BF16)

    def down(j):
        act, w = act_s[lax.rem(j, 2)], wd[lax.rem(j, 3)]
        acc[...] += dot(act, w) if n == 1 else dot_nt(act, w)

    zero = jnp.int32(0)
    start(zero)
    start(zero + 1)
    c_s[...] = rms(h_ref[...], gain_ref[...])
    acc[...] = h_ref[...].astype(F32)
    wait_gu(zero)
    gate_up(zero)

    def step(j, carry):
        @pl.when(j + 1 < steps)
        def _():
            start(j + 1)

        wait_gu(j)
        wait_dn(j - 1)
        gate_up(j)
        down(j - 1)
        return carry

    lax.fori_loop(1, steps, step, 0)
    wait_dn(zero + (steps - 1))
    down(zero + (steps - 1))
    out = acc[...].astype(BF16)
    out_ref[...] = rms(out, fin_ref[...]) if last else out


def mlp_block(h, gain, fin, w_gu, w_dn, layer, last, core):
    n = len(w_gu)
    t = h.shape[0]
    vm = pl.BlockSpec(memory_space=pltpu.VMEM)
    anym = pl.BlockSpec(memory_space=pl.ANY)
    return pl.pallas_call(
        functools.partial(mlp_kernel, n, layer, last),
        out_shape=jax.ShapeDtypeStruct((t, D), BF16),
        in_specs=[pl.BlockSpec(memory_space=pltpu.SMEM), vm, vm, vm] + [anym] * (2 * n),
        out_specs=vm,
        scratch_shapes=[
            pltpu.VMEM((2, D, FT), BF16), pltpu.VMEM((2, D, FT), BF16), pltpu.VMEM((3, FT, D) if n == 1 else (3, D, FT), BF16),
            pltpu.VMEM((t, D), BF16), pltpu.VMEM((2, t, FT), BF16), pltpu.VMEM((t, D), F32),
            pltpu.SemaphoreType.DMA((2, 4)), pltpu.SemaphoreType.DMA((3, 2)),
        ],
        compiler_params=pltpu.CompilerParams(vmem_limit_bytes=VMEM_LIMIT),
        cost_estimate=pl.CostEstimate(flops=6 * t * D * FF, bytes_accessed=6 * D * FF, transcendentals=0),
        name="mlp",
    )(core, h, gain, fin, *w_gu, *w_dn)


def gate_up_kernel(h_ref, gain_ref, wg_ref, wu_ref, act_ref, c_s):
    @pl.when(pl.program_id(0) == 0)
    def _():
        c_s[...] = rms(h_ref[...], gain_ref[...])

    g = dot(c_s[...], wg_ref[...])
    u = dot(c_s[...], wu_ref[...])
    act_ref[...] = (g * jax.nn.sigmoid(g) * u).astype(BF16)


def down_kernel(h_ref, act_ref, w_ref, fin_ref, out_ref, acc):
    j = pl.program_id(0)

    @pl.when(j == 0)
    def _():
        acc[...] = h_ref[...].astype(F32)

    acc[...] += dot(act_ref[...], w_ref[...])

    @pl.when(j == pl.num_programs(0) - 1)
    def _():
        out_ref[...] = rms(acc[...].astype(BF16), fin_ref[...])


def gate_up(h, gain, w_gu):
    t, steps = h.shape[0], FF // FT
    fixed = lambda j: (0, 0)
    return pl.pallas_call(
        gate_up_kernel,
        out_shape=jax.ShapeDtypeStruct((t, FF), BF16),
        grid=(steps,),
        in_specs=[
            pl.BlockSpec((t, D), fixed), pl.BlockSpec((1, D), fixed),
            pl.BlockSpec((D, FT), lambda j: (0, j)), pl.BlockSpec((D, FT), lambda j: (0, steps + j)),
        ],
        out_specs=pl.BlockSpec((t, FT), lambda j: (0, j)),
        scratch_shapes=[pltpu.VMEM((t, D), BF16)],
        compiler_params=pltpu.CompilerParams(vmem_limit_bytes=VMEM_LIMIT),
        cost_estimate=pl.CostEstimate(flops=4 * t * D * FF, bytes_accessed=4 * D * FF, transcendentals=0),
        name="gate_up",
    )(h, gain, w_gu, w_gu)


def down_norm(h, act, w_dn, fin):
    t = h.shape[0]
    fixed = lambda j: (0, 0)
    return pl.pallas_call(
        down_kernel,
        out_shape=jax.ShapeDtypeStruct((t, D), BF16),
        grid=(FF // FT,),
        in_specs=[
            pl.BlockSpec((t, D), fixed), pl.BlockSpec((t, FT), lambda j: (0, j)),
            pl.BlockSpec((FT, D), lambda j: (j, 0)), pl.BlockSpec((1, D), fixed),
        ],
        out_specs=pl.BlockSpec((t, D), fixed),
        scratch_shapes=[pltpu.VMEM((t, D), F32)],
        compiler_params=pltpu.CompilerParams(vmem_limit_bytes=VMEM_LIMIT),
        cost_estimate=pl.CostEstimate(flops=2 * t * D * FF, bytes_accessed=2 * D * FF, transcendentals=0),
        name="down",
    )(h, act, w_dn, fin)


def head_kernel(vocab, x_ref, w_ref, tgt_ref, out_ref, lg_s, m_s, s_s, p_s):
    j = pl.program_id(1)

    @pl.when(j == 0)
    def _():
        m_s[...] = jnp.full(m_s.shape, NEG, F32)
        s_s[...] = jnp.zeros(s_s.shape, F32)
        p_s[...] = jnp.zeros(p_s.shape, F32)

    lane = lax.broadcasted_iota(jnp.int32, m_s.shape, 1)
    rel = tgt_ref[...] - lane - j * VT
    held = vocab - j * VT

    def update(k):
        at = k * HT
        cols = [lg_s[k % 2, :, 128 * c:128 * (c + 1)] for c in range(HT // 128)]
        if at + HT > (vocab % VT or VT):
            cols = [jnp.where(lane < held - at - 128 * c, x, NEG) for c, x in enumerate(cols)]
        m_old = m_s[...]
        m_new = functools.reduce(jnp.maximum, cols, m_old)
        s_s[...] = s_s[...] * jnp.exp(m_old - m_new) + sum(jnp.exp(x - m_new) for x in cols)
        m_s[...] = m_new
        picked = 0.0
        for c, x in enumerate(cols):
            picked = jnp.where(rel == at + 128 * c, x, picked)
        p_s[...] += picked

    for k in range(VT // HT):
        lg_s[k % 2] = dot(x_ref[...], w_ref[:, k * HT:(k + 1) * HT])
        if k:
            update(k - 1)
    update(VT // HT - 1)

    @pl.when(j == pl.num_programs(1) - 1)
    def _():
        m = m_s[...]
        top = jnp.max(m, axis=1, keepdims=True)
        lse = top + jnp.log(jnp.sum(s_s[...] * jnp.exp(m - top), axis=1, keepdims=True))
        picked = jnp.sum(p_s[...], axis=1, keepdims=True)
        out_ref[...] = jnp.where(lane == 0, lse, picked)


def head_block(x, w, tgt, tt=1024):
    t, v = x.shape[0], w.shape[1]
    tgt = jnp.broadcast_to(jnp.where((tgt >= 0) & (tgt < v), tgt, -1)[:, None], (t, 128))
    out = pl.pallas_call(
        functools.partial(head_kernel, v),
        out_shape=jax.ShapeDtypeStruct((t, 128), F32),
        grid=(t // tt, pl.cdiv(v, VT)),
        in_specs=[
            pl.BlockSpec((tt, D), lambda i, j: (i, 0)), pl.BlockSpec((D, VT), lambda i, j: (0, j)),
            pl.BlockSpec((tt, 128), lambda i, j: (i, 0)),
        ],
        out_specs=pl.BlockSpec((tt, 128), lambda i, j: (i, 0)),
        scratch_shapes=[pltpu.VMEM((2, tt, HT), F32)] + [pltpu.VMEM((tt, 128), F32)] * 3,
        compiler_params=pltpu.CompilerParams(vmem_limit_bytes=VMEM_LIMIT),
        cost_estimate=pl.CostEstimate(flops=2 * t * D * v, bytes_accessed=2 * D * (v * t // tt + t), transcendentals=t * v),
        name="head",
    )(x, w, tgt)
    return out[:, 0], out[:, 1]


def rope_tables():
    half = HEAD_DIM // 2
    inv_freq = ROPE_BASE ** (-jnp.arange(half, dtype=F32) / half)
    angles = jnp.arange(SEQ, dtype=F32)[:, None] * inv_freq[None, :]
    cos, sin = jnp.cos(angles), jnp.sin(angles)
    cos = jnp.tile(jnp.concatenate([cos, cos] * 2, axis=1), (TB // SEQ, 1))
    sin = jnp.tile(jnp.concatenate([-sin, sin] * 2, axis=1), (TB // SEQ, 1))
    return cos, sin


def running_count(flags):
    n = flags.shape[-1]
    upper = (jnp.arange(n)[:, None] <= jnp.arange(n)[None, :]).astype(BF16)
    return dot(flags.astype(BF16), upper).astype(jnp.int32)


def relayout_kernel(w_ref, out_ref):
    for at in range(0, RT, 256):
        n = min(256, RT - at)
        eye = (lax.broadcasted_iota(jnp.int32, (n, n), 0) == lax.broadcasted_iota(jnp.int32, (n, n), 1)).astype(BF16)
        out_ref[at:at + n, :] = dot_nt(eye, w_ref[:, at:at + n]).astype(BF16)


def row_major(table_t):
    v = table_t.shape[1]
    return pl.pallas_call(
        relayout_kernel,
        out_shape=jax.ShapeDtypeStruct((v, D), BF16),
        grid=(v // RT,),
        in_specs=[pl.BlockSpec((D, RT), lambda j: (0, j))],
        out_specs=pl.BlockSpec((RT, D), lambda j: (j, 0)),
        compiler_params=pltpu.CompilerParams(vmem_limit_bytes=VMEM_LIMIT),
        cost_estimate=pl.CostEstimate(flops=2 * v * D * 256, bytes_accessed=4 * v * D, transcendentals=0),
        name="row_major",
    )(table_t)


def embed_send(table, toks, me, cap, r):
    size, vocab = toks.shape[0], table.shape[0]
    local = toks - me * vocab
    owned = (local >= 0) & (local < vocab)
    rank = running_count(owned) - 1
    slots = r * cap + jnp.arange(cap)
    hit = owned[:, None, :] & (rank[:, None, :] == slots[None, :, None])
    idx = jnp.sum(jnp.where(hit, local[:, None, :], 0), axis=2)
    rows = jnp.take(table, idx.reshape(-1), axis=0).reshape(size, cap, D)
    return [rows[k] for k in range(size)]


def embed_swap(rows, perms, axis):
    return rows[:1] + [lax.ppermute(rows[k], axis, perms[k]) for k in range(1, len(rows))]


def embed_pick(got, tok, vocab, me, cap, r):
    size, t = len(got), tok.shape[0]
    peers = jnp.bitwise_xor(me, jnp.arange(size))
    wanted = (tok // vocab)[None, :] == peers[:, None]
    slot = running_count(wanted) - 1 - r * cap
    pick = wanted[:, :, None] & (slot[:, :, None] == jnp.arange(cap)[None, None, :])
    pick = jnp.swapaxes(pick, 0, 1).reshape(t, size * cap).astype(BF16)
    return dot(pick, jnp.concatenate(got, axis=0)).astype(BF16)


def advantages(rewards, groups):
    same = (groups[:, None] == groups[None, :]).astype(F32)
    counts = jnp.sum(same, axis=1)
    means = jnp.sum(same * rewards[None, :], axis=1) / counts
    centred = rewards - means
    spread = jnp.sqrt(jnp.sum(same * (centred * centred)[None, :], axis=1) / counts)
    return centred / (spread + ADV_EPS)


def row_losses(logp, logp_ref, logp_old, weights, advantage):
    log_gap = logp_ref - logp
    kl_est = jnp.exp(log_gap) - log_gap - 1.0
    ratio = jnp.exp(logp - logp_old)
    adv_row = advantage[:, None]
    surrogate = jnp.minimum(ratio * adv_row, jnp.clip(ratio, 1.0 - CLIP_EPS, 1.0 + CLIP_EPS) * adv_row)
    per_token = -surrogate + BETA * kl_est
    return jnp.sum(per_token * weights, axis=1) / jnp.sum(weights, axis=1)


def solution(mesh):
    both = ('rep', 'fsdp')
    row_spec = P(both, None)
    n_dev = mesh.shape['rep'] * mesh.shape['fsdp']
    swap = [(0, 1), (1, 0)]
    xors = [[(d, d ^ k) for d in range(n_dev)] for k in range(n_dev)]

    def weight_specs(axes):
        return [P(None, axes, None)] * 5 + [P(None, axes), P(axes, None), P(axes, None)]

    in_specs = tuple([row_spec, row_spec, row_spec, P(both), P(both)] + weight_specs('fsdp') + weight_specs(both))
    out_specs = (P(), row_spec, row_spec)

    def device_step(tokens, resp_mask, logp_old, rewards, group_id, *weights):
        p_q, p_kv, p_o, p_gu, p_dn, p_norms, p_embed, p_head = weights[:8]
        r_q, r_kv, r_o, r_gu, r_dn, r_norms, r_embed, r_head = weights[8:]
        core = lax.axis_index('fsdp')
        me = lax.axis_index('rep') * 2 + core
        core_arr = core.astype(jnp.int32).reshape(1)
        rows = tokens.shape[0]
        t = rows * SEQ
        layers = p_q.shape[0]
        tabs = rope_tables()

        tok = tokens.reshape(t)
        tok_pair = jnp.stack([tok, lax.ppermute(tok, 'fsdp', swap)])
        local = tok_pair - core * p_embed.shape[0]
        index = jnp.clip(local, 0, p_embed.shape[0] - 1)
        table = row_major(p_embed.T)
        for_peer = jnp.take(table, index[1], axis=0)
        from_peer = lax.ppermute(for_peer, 'fsdp', swap)
        index, for_peer = lax.optimization_barrier((index[0], for_peer))
        for_own = jnp.take(table, index, axis=0)
        p_gains = jnp.stack([p_norms, lax.ppermute(p_norms, 'fsdp', swap)]).astype(F32)
        p_gains = jnp.where(core == 0, p_gains, p_gains[::-1])
        p_gains = jnp.swapaxes(p_gains, 0, 1).reshape(2 * layers + 1, 1, D)

        smalls = (tokens, resp_mask, logp_old, rewards, group_id, r_norms)
        small = jnp.concatenate([x.astype(F32).reshape(-1) for x in smalls])
        small = jnp.pad(small, (0, -small.size % 1024)).reshape(-1, 128)
        small = jnp.stack([small] + [lax.ppermute(small, both, xors[k]) for k in range(1, n_dev)])
        xor_ids = jnp.bitwise_xor(me, jnp.arange(n_dev))
        order = small.reshape(n_dev, -1)[:, :t].astype(jnp.int32)
        small = small[xor_ids].reshape(n_dev, -1)
        cuts, at = [], 0
        for x in smalls:
            cuts.append(small[:, at:at + x.size].reshape((n_dev,) + x.shape))
            at += x.size
        tok_all = cuts[0].astype(jnp.int32).reshape(n_dev, t)
        mask_all, old_all = (x.reshape(n_dev * rows, SEQ) for x in cuts[1:3])
        reward_all = cuts[3].reshape(-1)
        group_all = cuts[4].reshape(-1)
        r_gains = jnp.swapaxes(cuts[5], 0, 1).reshape(2 * layers + 1, 1, D)
        tgt_all = jnp.roll(tok_all.reshape(n_dev * rows, SEQ), -1, axis=1).reshape(n_dev, t)

        def attention_weights(q, kv, o):
            return jnp.concatenate([q, kv, jnp.zeros(q.shape[:-1] + (O_AT - QKV,), BF16), o], axis=-1)

        p_att = attention_weights(p_q, p_kv, p_o)
        p_parts = []
        for w in (p_att, p_gu, jnp.swapaxes(p_dn, 1, 2)):
            p_parts.append([w, lax.ppermute(w, 'fsdp', swap)])
        p_att, p_wgu, p_wdn = p_parts
        p_head, r_head = p_head.T, r_head.T

        def ref_weights(layer, dn):
            att = attention_weights(r_q[layer], r_kv[layer], r_o[layer])
            return [lax.all_gather(w, both, axis=0, tiled=True) for w in (att, r_gu[layer], dn)]

        def policy_layer(h, layer):
            h = attention_block(h, p_gains[2 * layer], tabs, p_att, layer, core_arr)
            return mlp_block(h, p_gains[2 * layer + 1], p_gains[2 * layers], p_wgu, p_wdn, layer, layer == layers - 1, core_arr)

        r_full = [ref_weights(0, r_dn[0])]
        cap = 192
        order, for_own = lax.optimization_barrier((order, for_own))
        for_own, got = lax.optimization_barrier((for_own, embed_send(r_embed, order, me, cap, 0)))
        got = embed_swap(got, xors, both)
        h = jnp.where(((local[0] >= 0) & (local[0] < p_embed.shape[0]))[:, None], for_own, from_peer)
        h = policy_layer(h, 0)
        got, dn, h = lax.optimization_barrier((got, r_dn[1], h))
        r_full.append(ref_weights(1, dn))
        h_ref = embed_pick(got, tok, r_embed.shape[0], me, cap, 0)
        counts = jnp.sum((tok_all[:, None, :] // r_embed.shape[0]) == jnp.arange(n_dev)[None, :, None], axis=2)
        h_ref = lax.fori_loop(1, (jnp.max(counts) + cap - 1) // cap, lambda r, acc: acc + embed_pick(
            embed_swap(embed_send(r_embed, order, me, cap, r), xors, both), tok, r_embed.shape[0], me, cap, r), h_ref)
        tgt_own = tgt_all[me] - core * p_head.shape[1]
        tgt_peer = tgt_all[jnp.bitwise_xor(me, 1)] - core * p_head.shape[1]

        h_ref, h = lax.optimization_barrier((h_ref, h))
        att, w_gu, w_dn = r_full[0]
        h_ref = attention_block(h_ref, r_gains[0], tabs, [att], None, core_arr)
        h_ref = mlp_block(h_ref, r_gains[1], r_gains[2 * layers], [w_gu], [w_dn], None, False, core_arr)
        h, h_ref = lax.optimization_barrier((h, h_ref))
        x = policy_layer(h, 1)
        x_peer = lax.ppermute(x, 'fsdp', swap)
        own = head_block(x, p_head, tgt_own)
        h_ref, own = lax.optimization_barrier((h_ref, own))
        att, w_gu, w_dn = r_full[1]
        h_ref = attention_block(h_ref, r_gains[2], tabs, [att], None, core_arr)
        act = gate_up(h_ref, r_gains[3], w_gu)
        x_ref = down_norm(h_ref, act, w_dn, r_gains[2 * layers])
        x_peer, x_ref = lax.optimization_barrier((x_peer, x_ref))
        x_all = [lax.all_gather(x_ref[at:at + t // 2], both, axis=0, tiled=True) for at in (0, t // 2)]
        peer = head_block(x_peer, p_head, tgt_peer)

        x_all[0], peer = lax.optimization_barrier((x_all[0], peer))
        parts = [jnp.stack(own + peer)]
        for half in range(2):
            tgt = tgt_all[:, half * (t // 2):(half + 1) * (t // 2)].reshape(-1) - me * r_head.shape[1]
            parts += [out.reshape(n_dev // 2, t) for out in head_block(x_all[half], r_head, tgt)]
        parts = lax.all_gather(jnp.concatenate(parts, axis=0), both)
        p_part = parts[:, :4]
        r_part = parts[:, 4:].reshape(n_dev, 2, 2, n_dev, t // 2)
        r_part = jnp.transpose(r_part, (2, 0, 3, 1, 4)).reshape(2, n_dev, n_dev, t)

        def finish(lse, picked):
            next_lp = (jnp.sum(picked, axis=0) - jax.nn.logsumexp(lse, axis=0)).reshape(n_dev * rows, SEQ)
            return jnp.where(jnp.arange(SEQ)[None, :] == 0, 0.0, jnp.roll(next_lp, 1, axis=1))

        logp_ref = finish(r_part[0], r_part[1])
        by_peer = p_part.reshape(n_dev // 2, 2, 4, t)[:, ::-1].reshape(n_dev, 4, t)
        lse = jnp.stack([p_part[:, 0], by_peer[:, 2]])
        picked = jnp.stack([p_part[:, 1], by_peer[:, 3]])
        logp = finish(lse, picked)
        row_part = row_losses(logp, logp_ref, old_all, mask_all, advantages(reward_all, group_all))
        loss = jnp.sum(row_part) / row_part.shape[0]
        return loss, lax.dynamic_slice_in_dim(logp, me * rows, rows), lax.dynamic_slice_in_dim(logp_ref, me * rows, rows)

    return jax.shard_map(device_step, mesh=mesh, in_specs=in_specs, out_specs=out_specs, check_vma=False)
```

```python
import functools

import jax
import jax.numpy as jnp
from jax import lax
from jax.experimental import pallas as pl
from jax.experimental.pallas import tpu as pltpu
from jax.sharding import PartitionSpec as P


HEAD_DIM = 64
EPS = 1e-6
ROPE_BASE = 10000.0
CLIP_EPS = 0.2
BETA = 0.04
ADV_EPS = 1e-4

F32 = jnp.float32
BF16 = jnp.bfloat16
NEG = -3.0e38
VMEM_LIMIT = 62 * 1024 * 1024

D = 1600
QH = 25
KVH = 5
QKV = 2240
O_AT = 2304
FF = 4352
SEQ = 32
TB = 256
SUB = 128
FT = 256
RT = 640
VT = 2048
HT = 512


def dot(lhs, rhs):
    return lax.dot_general(lhs, rhs, (((1,), (0,)), ((), ())), preferred_element_type=F32)


def dot_nt(lhs, rhs):
    return lax.dot_general(lhs, rhs, (((1,), (1,)), ((), ())), preferred_element_type=F32)


def dot_tn(lhs, rhs):
    return lax.dot_general(lhs, rhs, (((0,), (0,)), ((), ())), preferred_element_type=F32)


def rms(x, gain):
    x = x.astype(F32)
    inv = lax.rsqrt(jnp.sum(x * x, axis=-1, keepdims=True) * (1.0 / D) + EPS)
    return (x * inv * gain).astype(BF16)


def row_copies(parts, layer, half_of, dst, sems, base):
    out = []
    for p, part in enumerate(parts):
        src = part if layer is None else part.at[layer]
        rows = src.shape[0]
        at = pl.multiple_of(half_of(p) * rows, 8) if len(parts) > 1 else 0
        out.append(pltpu.make_async_copy(src, dst.at[pl.ds(at, rows)], sems.at[base + p]))
    return out


def attn_kernel(n, layer, core_ref, h_ref, gain_ref, cos_ref, sin_ref, *refs):
    out_ref, w_s, qkv_s, qk_s, o_s, sc_s, p_s, sems = refs[n:]
    core = core_ref[0]

    def half_of(p):
        return jnp.bitwise_xor(core, p)

    copies = row_copies(refs[:n], layer, half_of, w_s, sems, 0)
    for copy in copies:
        copy.start()
    for copy in copies:
        copy.wait()

    lane = lax.broadcasted_iota(jnp.int32, (1, 128), 1)
    low_half = lane < 64
    rot_mask = (lane % 64) < 32
    k_idx = lax.broadcasted_iota(jnp.int32, (2 * SUB, SUB), 0) % SUB
    q_idx = lax.broadcasted_iota(jnp.int32, (2 * SUB, SUB), 1)
    keep = (q_idx // SEQ == k_idx // SEQ) & (k_idx <= q_idx)
    blank = jnp.zeros((HEAD_DIM, SUB), F32)

    def project(b):
        rows = pl.ds(pl.multiple_of(b * TB, TB), TB)
        qkv_s[...] = dot(rms(h_ref[rows, :], gain_ref[...]), w_s[:, :QKV])
        cos, sin = cos_ref[...], sin_ref[...]
        for j in range(15):
            x = qkv_s[:, 128 * j:128 * (j + 1)]
            rot = jnp.where(rot_mask, pltpu.roll(x, 96, 1), pltpu.roll(x, 32, 1))
            qk_s[:, 128 * j:128 * (j + 1)] = (x * cos + rot * sin).astype(BF16)

    def attend(s):
        rows = slice(s * SUB, (s + 1) * SUB)
        k_pads, v_pads = [], []
        for g in range(KVH):
            c, side = divmod(25 + g, 2)
            x = qk_s[rows, 128 * c:128 * (c + 1)].astype(F32)
            y = pltpu.roll(x, 64, 1)
            at_low, at_high = (y, x) if side else (x, y)
            k_pads.append((jnp.where(low_half, at_low, 0.0).astype(BF16), jnp.where(low_half, 0.0, at_high).astype(BF16)))
        for c in range(3):
            if c < 2:
                x = qkv_s[rows, 1920 + 128 * c:2048 + 128 * c]
            else:
                x = jnp.concatenate([qkv_s[rows, 2176:2240], jnp.zeros((SUB, 64), F32)], axis=1)
            x = x.T
            for side in range(2 if c < 2 else 1):
                v = x[64 * side:64 * (side + 1)]
                v_pads.append((jnp.concatenate([v, blank], axis=0).astype(BF16), jnp.concatenate([blank, v], axis=0).astype(BF16)))
        heads = [((2 * j) // 5, min((2 * j + 1) // 5, KVH - 1)) for j in range(13)]
        for j, (ga, gb) in enumerate(heads):
            keys = jnp.concatenate([k_pads[ga][0], k_pads[gb][1]], axis=0)
            scores = dot_nt(keys, qk_s[rows, 128 * j:128 * (j + 1)]) * (HEAD_DIM ** -0.5)
            sc_s[2 * SUB * j:2 * SUB * (j + 1), :] = jnp.where(keep, scores, -1e30)
        for i in range(QH):
            x = sc_s[SUB * i:SUB * (i + 1), :]
            e = jnp.exp(x - jnp.max(x, axis=0, keepdims=True))
            p_s[SUB * i:SUB * (i + 1), :] = (e * (1.0 / jnp.sum(e, axis=0, keepdims=True))).astype(BF16)
        for j, (ga, gb) in enumerate(heads):
            if j < 12:
                vals = jnp.concatenate([v_pads[ga][0], v_pads[gb][1]], axis=1)
                o_s[128 * j:128 * (j + 1), rows] = dot(vals, p_s[2 * SUB * j:2 * SUB * (j + 1), :]).astype(BF16)
            else:
                o_s[1536:1600, rows] = dot(v_pads[ga][0], p_s[2 * SUB * j:2 * SUB * j + SUB, :])[:64].astype(BF16)

    def block(b, carry):
        rows = pl.ds(pl.multiple_of(b * TB, TB), TB)
        project(b)
        for s in range(TB // SUB):
            attend(s)
        out_ref[rows, :] = (h_ref[rows, :].astype(F32) + dot_tn(o_s[...], w_s[:, O_AT:])).astype(BF16)
        return carry

    lax.fori_loop(0, h_ref.shape[0] // TB, block, 0)


def attention_block(h, gain, tabs, w_att, layer, core):
    n = len(w_att)
    t = h.shape[0]
    vm = pl.BlockSpec(memory_space=pltpu.VMEM)
    anym = pl.BlockSpec(memory_space=pl.ANY)
    return pl.pallas_call(
        functools.partial(attn_kernel, n, layer),
        out_shape=jax.ShapeDtypeStruct((t, D), BF16),
        in_specs=[pl.BlockSpec(memory_space=pltpu.SMEM), vm, vm, vm, vm] + [anym] * n,
        out_specs=vm,
        scratch_shapes=[
            pltpu.VMEM((D, O_AT + D), BF16), pltpu.VMEM((TB, QKV), F32),
            pltpu.VMEM((TB, 1920), BF16), pltpu.VMEM((D, TB), BF16), pltpu.VMEM((26 * SUB, SUB), F32), pltpu.VMEM((26 * SUB, SUB), BF16),
            pltpu.SemaphoreType.DMA((n,)),
        ],
        compiler_params=pltpu.CompilerParams(vmem_limit_bytes=VMEM_LIMIT),
        cost_estimate=pl.CostEstimate(flops=2 * t * D * (QKV + D), bytes_accessed=2 * D * (QKV + D), transcendentals=0),
        name="attn",
    )(core, h, gain, tabs[0], tabs[1], *w_att)


def mlp_kernel(n, layer, last, core_ref, h_ref, gain_ref, fin_ref, *refs):
    gu_parts, dn_parts = refs[:n], refs[n:2 * n]
    out_ref, wg, wu, wd, c_s, act_s, acc, sems, dn_sems = refs[2 * n:]
    core = core_ref[0]
    steps = FF // FT
    half_subs = FF // 2 // 128

    def gu_copies(j, slot):
        out = []
        for p, part in enumerate(gu_parts):
            src = part if layer is None else part.at[layer]
            rows = src.shape[0]
            at = pl.multiple_of(jnp.bitwise_xor(core, p) * rows, 8) if n > 1 else 0
            for t, dst in enumerate((wg, wu)):
                cols = pl.ds(pl.multiple_of(t * FF + j * FT, 128), FT)
                out.append(pltpu.make_async_copy(src.at[:, cols], dst.at[slot, pl.ds(at, rows)], sems.at[slot, 2 * p + t]))
        return out

    def dn_copy(part, j, i):
        slot = lax.rem(j, 3)
        src = part if layer is None else part.at[layer]
        if n == 1:
            at = pl.multiple_of(j * FT, FT)
            return pltpu.make_async_copy(src.at[pl.ds(at, FT)], wd.at[slot], dn_sems.at[slot, 0])
        sub = 2 * j + i
        col = pl.multiple_of(jnp.where(sub >= half_subs, sub - half_subs, sub) * 128, 128)
        return pltpu.make_async_copy(src.at[:, pl.ds(col, 128)], wd.at[slot, :, pl.ds(128 * i, 128)], dn_sems.at[slot, i])

    def start(j):
        for copy in gu_copies(j, lax.rem(j, 2)):
            copy.start()
        if n == 1:
            dn_copy(dn_parts[0], j, 0).start()
        else:
            for i in range(2):
                half = (2 * j + i >= half_subs).astype(jnp.int32)
                mine = half == core

                @pl.when(mine)
                def _():
                    dn_copy(dn_parts[0], j, i).start()

                @pl.when(jnp.logical_not(mine))
                def _():
                    dn_copy(dn_parts[1], j, i).start()

    def wait_gu(j):
        for copy in gu_copies(j, lax.rem(j, 2)):
            copy.wait()

    def wait_dn(j):
        for i in range(n):
            dn_copy(dn_parts[0], j, i).wait()

    def gate_up(j):
        slot = lax.rem(j, 2)
        g = dot(c_s[...], wg[slot])
        u = dot(c_s[...], wu[slot])
        act_s[slot] = (g * jax.nn.sigmoid(g) * u).astype(BF16)

    def down(j):
        act, w = act_s[lax.rem(j, 2)], wd[lax.rem(j, 3)]
        acc[...] += dot(act, w) if n == 1 else dot_nt(act, w)

    zero = jnp.int32(0)
    start(zero)
    start(zero + 1)
    c_s[...] = rms(h_ref[...], gain_ref[...])
    acc[...] = h_ref[...].astype(F32)
    wait_gu(zero)
    gate_up(zero)

    def step(j, carry):
        @pl.when(j + 1 < steps)
        def _():
            start(j + 1)

        wait_gu(j)
        wait_dn(j - 1)
        gate_up(j)
        down(j - 1)
        return carry

    lax.fori_loop(1, steps, step, 0)
    wait_dn(zero + (steps - 1))
    down(zero + (steps - 1))
    out = acc[...].astype(BF16)
    out_ref[...] = rms(out, fin_ref[...]) if last else out


def mlp_block(h, gain, fin, w_gu, w_dn, layer, last, core):
    n = len(w_gu)
    t = h.shape[0]
    vm = pl.BlockSpec(memory_space=pltpu.VMEM)
    anym = pl.BlockSpec(memory_space=pl.ANY)
    return pl.pallas_call(
        functools.partial(mlp_kernel, n, layer, last),
        out_shape=jax.ShapeDtypeStruct((t, D), BF16),
        in_specs=[pl.BlockSpec(memory_space=pltpu.SMEM), vm, vm, vm] + [anym] * (2 * n),
        out_specs=vm,
        scratch_shapes=[
            pltpu.VMEM((2, D, FT), BF16), pltpu.VMEM((2, D, FT), BF16), pltpu.VMEM((3, FT, D) if n == 1 else (3, D, FT), BF16),
            pltpu.VMEM((t, D), BF16), pltpu.VMEM((2, t, FT), BF16), pltpu.VMEM((t, D), F32),
            pltpu.SemaphoreType.DMA((2, 4)), pltpu.SemaphoreType.DMA((3, 2)),
        ],
        compiler_params=pltpu.CompilerParams(vmem_limit_bytes=VMEM_LIMIT),
        cost_estimate=pl.CostEstimate(flops=6 * t * D * FF, bytes_accessed=6 * D * FF, transcendentals=0),
        name="mlp",
    )(core, h, gain, fin, *w_gu, *w_dn)


def gate_up_kernel(h_ref, gain_ref, wg_ref, wu_ref, act_ref, c_s):
    @pl.when(pl.program_id(0) == 0)
    def _():
        c_s[...] = rms(h_ref[...], gain_ref[...])

    g = dot(c_s[...], wg_ref[...])
    u = dot(c_s[...], wu_ref[...])
    act_ref[...] = (g * jax.nn.sigmoid(g) * u).astype(BF16)


def down_kernel(h_ref, act_ref, w_ref, fin_ref, out_ref, acc):
    j = pl.program_id(0)

    @pl.when(j == 0)
    def _():
        acc[...] = h_ref[...].astype(F32)

    acc[...] += dot(act_ref[...], w_ref[...])

    @pl.when(j == pl.num_programs(0) - 1)
    def _():
        out_ref[...] = rms(acc[...].astype(BF16), fin_ref[...])


def gate_up(h, gain, w_gu):
    t, steps = h.shape[0], FF // FT
    fixed = lambda j: (0, 0)
    return pl.pallas_call(
        gate_up_kernel,
        out_shape=jax.ShapeDtypeStruct((t, FF), BF16),
        grid=(steps,),
        in_specs=[
            pl.BlockSpec((t, D), fixed), pl.BlockSpec((1, D), fixed),
            pl.BlockSpec((D, FT), lambda j: (0, j)), pl.BlockSpec((D, FT), lambda j: (0, steps + j)),
        ],
        out_specs=pl.BlockSpec((t, FT), lambda j: (0, j)),
        scratch_shapes=[pltpu.VMEM((t, D), BF16)],
        compiler_params=pltpu.CompilerParams(vmem_limit_bytes=VMEM_LIMIT),
        cost_estimate=pl.CostEstimate(flops=4 * t * D * FF, bytes_accessed=4 * D * FF, transcendentals=0),
        name="gate_up",
    )(h, gain, w_gu, w_gu)


def down_norm(h, act, w_dn, fin):
    t = h.shape[0]
    fixed = lambda j: (0, 0)
    return pl.pallas_call(
        down_kernel,
        out_shape=jax.ShapeDtypeStruct((t, D), BF16),
        grid=(FF // FT,),
        in_specs=[
            pl.BlockSpec((t, D), fixed), pl.BlockSpec((t, FT), lambda j: (0, j)),
            pl.BlockSpec((FT, D), lambda j: (j, 0)), pl.BlockSpec((1, D), fixed),
        ],
        out_specs=pl.BlockSpec((t, D), fixed),
        scratch_shapes=[pltpu.VMEM((t, D), F32)],
        compiler_params=pltpu.CompilerParams(vmem_limit_bytes=VMEM_LIMIT),
        cost_estimate=pl.CostEstimate(flops=2 * t * D * FF, bytes_accessed=2 * D * FF, transcendentals=0),
        name="down",
    )(h, act, w_dn, fin)


def head_kernel(vocab, x_ref, w_ref, tgt_ref, out_ref, lg_s, m_s, s_s, p_s):
    j = pl.program_id(1)

    @pl.when(j == 0)
    def _():
        m_s[...] = jnp.full(m_s.shape, NEG, F32)
        s_s[...] = jnp.zeros(s_s.shape, F32)
        p_s[...] = jnp.zeros(p_s.shape, F32)

    lane = lax.broadcasted_iota(jnp.int32, m_s.shape, 1)
    rel = tgt_ref[...] - lane - j * VT
    held = vocab - j * VT

    def update(k):
        at = k * HT
        cols = [lg_s[k % 2, :, 128 * c:128 * (c + 1)] for c in range(HT // 128)]
        if at + HT > (vocab % VT or VT):
            cols = [jnp.where(lane < held - at - 128 * c, x, NEG) for c, x in enumerate(cols)]
        m_old = m_s[...]
        m_new = functools.reduce(jnp.maximum, cols, m_old)
        s_s[...] = s_s[...] * jnp.exp(m_old - m_new) + sum(jnp.exp(x - m_new) for x in cols)
        m_s[...] = m_new
        picked = 0.0
        for c, x in enumerate(cols):
            picked = jnp.where(rel == at + 128 * c, x, picked)
        p_s[...] += picked

    for k in range(VT // HT):
        lg_s[k % 2] = dot(x_ref[...], w_ref[:, k * HT:(k + 1) * HT])
        if k:
            update(k - 1)
    update(VT // HT - 1)

    @pl.when(j == pl.num_programs(1) - 1)
    def _():
        m = m_s[...]
        top = jnp.max(m, axis=1, keepdims=True)
        lse = top + jnp.log(jnp.sum(s_s[...] * jnp.exp(m - top), axis=1, keepdims=True))
        picked = jnp.sum(p_s[...], axis=1, keepdims=True)
        out_ref[...] = jnp.where(lane == 0, lse, picked)


def head_block(x, w, tgt, tt=1024):
    t, v = x.shape[0], w.shape[1]
    tgt = jnp.broadcast_to(jnp.where((tgt >= 0) & (tgt < v), tgt, -1)[:, None], (t, 128))
    out = pl.pallas_call(
        functools.partial(head_kernel, v),
        out_shape=jax.ShapeDtypeStruct((t, 128), F32),
        grid=(t // tt, pl.cdiv(v, VT)),
        in_specs=[
            pl.BlockSpec((tt, D), lambda i, j: (i, 0)), pl.BlockSpec((D, VT), lambda i, j: (0, j)),
            pl.BlockSpec((tt, 128), lambda i, j: (i, 0)),
        ],
        out_specs=pl.BlockSpec((tt, 128), lambda i, j: (i, 0)),
        scratch_shapes=[pltpu.VMEM((2, tt, HT), F32)] + [pltpu.VMEM((tt, 128), F32)] * 3,
        compiler_params=pltpu.CompilerParams(vmem_limit_bytes=VMEM_LIMIT),
        cost_estimate=pl.CostEstimate(flops=2 * t * D * v, bytes_accessed=2 * D * (v * t // tt + t), transcendentals=t * v),
        name="head",
    )(x, w, tgt)
    return out[:, 0], out[:, 1]


def rope_tables():
    half = HEAD_DIM // 2
    inv_freq = ROPE_BASE ** (-jnp.arange(half, dtype=F32) / half)
    angles = jnp.arange(SEQ, dtype=F32)[:, None] * inv_freq[None, :]
    cos, sin = jnp.cos(angles), jnp.sin(angles)
    cos = jnp.tile(jnp.concatenate([cos, cos] * 2, axis=1), (TB // SEQ, 1))
    sin = jnp.tile(jnp.concatenate([-sin, sin] * 2, axis=1), (TB // SEQ, 1))
    return cos, sin


def running_count(flags):
    n = flags.shape[-1]
    upper = (jnp.arange(n)[:, None] <= jnp.arange(n)[None, :]).astype(BF16)
    return dot(flags.astype(BF16), upper).astype(jnp.int32)


def relayout_kernel(w_ref, out_ref):
    for at in range(0, RT, 256):
        n = min(256, RT - at)
        eye = (lax.broadcasted_iota(jnp.int32, (n, n), 0) == lax.broadcasted_iota(jnp.int32, (n, n), 1)).astype(BF16)
        out_ref[at:at + n, :] = dot_nt(eye, w_ref[:, at:at + n]).astype(BF16)


def row_major(table_t):
    v = table_t.shape[1]
    return pl.pallas_call(
        relayout_kernel,
        out_shape=jax.ShapeDtypeStruct((v, D), BF16),
        grid=(v // RT,),
        in_specs=[pl.BlockSpec((D, RT), lambda j: (0, j))],
        out_specs=pl.BlockSpec((RT, D), lambda j: (j, 0)),
        compiler_params=pltpu.CompilerParams(vmem_limit_bytes=VMEM_LIMIT),
        cost_estimate=pl.CostEstimate(flops=2 * v * D * 256, bytes_accessed=4 * v * D, transcendentals=0),
        name="row_major",
    )(table_t)


def take_rows(table, index):
    parts = [table.at[part].get(mode='promise_in_bounds') for part in jnp.split(index, index.shape[0] // 512)]
    return jnp.concatenate(parts, axis=0)


def embed_send(table, toks, me, cap, r):
    size, vocab = toks.shape[0], table.shape[0]
    local = toks - me * vocab
    owned = (local >= 0) & (local < vocab)
    rank = running_count(owned) - 1
    slots = r * cap + jnp.arange(cap)
    hit = owned[:, None, :] & (rank[:, None, :] == slots[None, :, None])
    idx = jnp.sum(jnp.where(hit, local[:, None, :], 0), axis=2)
    rows = table.at[idx.reshape(-1)].get(mode='promise_in_bounds').reshape(size, cap, D)
    return [rows[k] for k in range(size)]


def embed_swap(rows, perms, axis):
    return rows[:1] + [lax.ppermute(rows[k], axis, perms[k]) for k in range(1, len(rows))]


def embed_pick(got, tok, vocab, me, cap, r):
    size, t = len(got), tok.shape[0]
    peers = jnp.bitwise_xor(me, jnp.arange(size))
    wanted = (tok // vocab)[None, :] == peers[:, None]
    slot = running_count(wanted) - 1 - r * cap
    pick = wanted[:, :, None] & (slot[:, :, None] == jnp.arange(cap)[None, None, :])
    pick = jnp.swapaxes(pick, 0, 1).reshape(t, size * cap).astype(BF16)
    return dot(pick, jnp.concatenate(got, axis=0)).astype(BF16)


def advantages(rewards, groups):
    same = (groups[:, None] == groups[None, :]).astype(F32)
    counts = jnp.sum(same, axis=1)
    means = jnp.sum(same * rewards[None, :], axis=1) / counts
    centred = rewards - means
    spread = jnp.sqrt(jnp.sum(same * (centred * centred)[None, :], axis=1) / counts)
    return centred / (spread + ADV_EPS)


def row_losses(logp, logp_ref, logp_old, weights, advantage):
    log_gap = logp_ref - logp
    kl_est = jnp.exp(log_gap) - log_gap - 1.0
    ratio = jnp.exp(logp - logp_old)
    adv_row = advantage[:, None]
    surrogate = jnp.minimum(ratio * adv_row, jnp.clip(ratio, 1.0 - CLIP_EPS, 1.0 + CLIP_EPS) * adv_row)
    per_token = -surrogate + BETA * kl_est
    return jnp.sum(per_token * weights, axis=1) / jnp.sum(weights, axis=1)


def solution(mesh):
    both = ('rep', 'fsdp')
    row_spec = P(both, None)
    n_dev = mesh.shape['rep'] * mesh.shape['fsdp']
    swap = [(0, 1), (1, 0)]
    xors = [[(d, d ^ k) for d in range(n_dev)] for k in range(n_dev)]

    def weight_specs(axes):
        return [P(None, axes, None)] * 5 + [P(None, axes), P(axes, None), P(axes, None)]

    in_specs = tuple([row_spec, row_spec, row_spec, P(both), P(both)] + weight_specs('fsdp') + weight_specs(both))
    out_specs = (P(), row_spec, row_spec)

    def device_step(tokens, resp_mask, logp_old, rewards, group_id, *weights):
        p_q, p_kv, p_o, p_gu, p_dn, p_norms, p_embed, p_head = weights[:8]
        r_q, r_kv, r_o, r_gu, r_dn, r_norms, r_embed, r_head = weights[8:]
        core = lax.axis_index('fsdp')
        me = lax.axis_index('rep') * 2 + core
        core_arr = core.astype(jnp.int32).reshape(1)
        rows = tokens.shape[0]
        t = rows * SEQ
        layers = p_q.shape[0]
        tabs = rope_tables()

        tok = tokens.reshape(t)
        tok_pair = jnp.stack([tok, lax.ppermute(tok, 'fsdp', swap)])
        local = tok_pair - core * p_embed.shape[0]
        index = jnp.clip(local, 0, p_embed.shape[0] - 1)
        table = row_major(p_embed.T)
        for_peer = take_rows(table, index[1])
        from_peer = lax.ppermute(for_peer, 'fsdp', swap)
        index, for_peer = lax.optimization_barrier((index[0], for_peer))
        for_own = take_rows(table, index)
        p_gains = jnp.stack([p_norms, lax.ppermute(p_norms, 'fsdp', swap)]).astype(F32)
        p_gains = jnp.where(core == 0, p_gains, p_gains[::-1])
        p_gains = jnp.swapaxes(p_gains, 0, 1).reshape(2 * layers + 1, 1, D)

        smalls = (tokens, resp_mask, logp_old, rewards, group_id, r_norms)
        small = jnp.concatenate([x.astype(F32).reshape(-1) for x in smalls])
        small = jnp.pad(small, (0, -small.size % 1024)).reshape(-1, 128)
        small = jnp.stack([small] + [lax.ppermute(small, both, xors[k]) for k in range(1, n_dev)])
        xor_ids = jnp.bitwise_xor(me, jnp.arange(n_dev))
        order = small.reshape(n_dev, -1)[:, :t].astype(jnp.int32)
        small = small[xor_ids].reshape(n_dev, -1)
        cuts, at = [], 0
        for x in smalls:
            cuts.append(small[:, at:at + x.size].reshape((n_dev,) + x.shape))
            at += x.size
        tok_all = cuts[0].astype(jnp.int32).reshape(n_dev, t)
        mask_all, old_all = (x.reshape(n_dev * rows, SEQ) for x in cuts[1:3])
        reward_all = cuts[3].reshape(-1)
        group_all = cuts[4].reshape(-1)
        r_gains = jnp.swapaxes(cuts[5], 0, 1).reshape(2 * layers + 1, 1, D)
        tgt_all = jnp.roll(tok_all.reshape(n_dev * rows, SEQ), -1, axis=1).reshape(n_dev, t)

        def attention_weights(q, kv, o):
            return jnp.concatenate([q, kv, jnp.zeros(q.shape[:-1] + (O_AT - QKV,), BF16), o], axis=-1)

        p_att = attention_weights(p_q, p_kv, p_o)
        p_parts = []
        for w in (p_att, p_gu, jnp.swapaxes(p_dn, 1, 2)):
            p_parts.append([w, lax.ppermute(w, 'fsdp', swap)])
        p_att, p_wgu, p_wdn = p_parts
        p_head, r_head = p_head.T, r_head.T

        def ref_weights(layer, dn):
            att = attention_weights(r_q[layer], r_kv[layer], r_o[layer])
            return [lax.all_gather(w, both, axis=0, tiled=True) for w in (att, r_gu[layer], dn)]

        def policy_layer(h, layer):
            h = attention_block(h, p_gains[2 * layer], tabs, p_att, layer, core_arr)
            return mlp_block(h, p_gains[2 * layer + 1], p_gains[2 * layers], p_wgu, p_wdn, layer, layer == layers - 1, core_arr)

        r_full = [ref_weights(0, r_dn[0])]
        cap = 192
        order, for_own = lax.optimization_barrier((order, for_own))
        for_own, got = lax.optimization_barrier((for_own, embed_send(r_embed, order, me, cap, 0)))
        got = embed_swap(got, xors, both)
        h = jnp.where(((local[0] >= 0) & (local[0] < p_embed.shape[0]))[:, None], for_own, from_peer)
        h = policy_layer(h, 0)
        got, dn, h = lax.optimization_barrier((got, r_dn[1], h))
        r_full.append(ref_weights(1, dn))
        h_ref = embed_pick(got, tok, r_embed.shape[0], me, cap, 0)
        counts = jnp.sum((tok_all[:, None, :] // r_embed.shape[0]) == jnp.arange(n_dev)[None, :, None], axis=2)
        h_ref = lax.fori_loop(1, (jnp.max(counts) + cap - 1) // cap, lambda r, acc: acc + embed_pick(
            embed_swap(embed_send(r_embed, order, me, cap, r), xors, both), tok, r_embed.shape[0], me, cap, r), h_ref)
        tgt_own = tgt_all[me] - core * p_head.shape[1]
        tgt_peer = tgt_all[jnp.bitwise_xor(me, 1)] - core * p_head.shape[1]

        h_ref, h = lax.optimization_barrier((h_ref, h))
        att, w_gu, w_dn = r_full[0]
        h_ref = attention_block(h_ref, r_gains[0], tabs, [att], None, core_arr)
        h_ref = mlp_block(h_ref, r_gains[1], r_gains[2 * layers], [w_gu], [w_dn], None, False, core_arr)
        h, h_ref = lax.optimization_barrier((h, h_ref))
        x = policy_layer(h, 1)
        x_peer = lax.ppermute(x, 'fsdp', swap)
        own = head_block(x, p_head, tgt_own)
        h_ref, own = lax.optimization_barrier((h_ref, own))
        att, w_gu, w_dn = r_full[1]
        h_ref = attention_block(h_ref, r_gains[2], tabs, [att], None, core_arr)
        act = gate_up(h_ref, r_gains[3], w_gu)
        x_ref = down_norm(h_ref, act, w_dn, r_gains[2 * layers])
        x_peer, x_ref = lax.optimization_barrier((x_peer, x_ref))
        x_all = [lax.all_gather(x_ref[at:at + t // 2], both, axis=0, tiled=True) for at in (0, t // 2)]
        peer = head_block(x_peer, p_head, tgt_peer)

        x_all[0], peer = lax.optimization_barrier((x_all[0], peer))
        parts = [jnp.stack(own + peer)]
        for half in range(2):
            tgt = tgt_all[:, half * (t // 2):(half + 1) * (t // 2)].reshape(-1) - me * r_head.shape[1]
            parts += [out.reshape(n_dev // 2, t) for out in head_block(x_all[half], r_head, tgt)]
        parts = lax.all_gather(jnp.concatenate(parts, axis=0), both)
        p_part = parts[:, :4]
        r_part = parts[:, 4:].reshape(n_dev, 2, 2, n_dev, t // 2)
        r_part = jnp.transpose(r_part, (2, 0, 3, 1, 4)).reshape(2, n_dev, n_dev, t)

        def finish(lse, picked):
            next_lp = (jnp.sum(picked, axis=0) - jax.nn.logsumexp(lse, axis=0)).reshape(n_dev * rows, SEQ)
            return jnp.where(jnp.arange(SEQ)[None, :] == 0, 0.0, jnp.roll(next_lp, 1, axis=1))

        logp_ref = finish(r_part[0], r_part[1])
        by_peer = p_part.reshape(n_dev // 2, 2, 4, t)[:, ::-1].reshape(n_dev, 4, t)
        lse = jnp.stack([p_part[:, 0], by_peer[:, 2]])
        picked = jnp.stack([p_part[:, 1], by_peer[:, 3]])
        logp = finish(lse, picked)
        row_part = row_losses(logp, logp_ref, old_all, mask_all, advantages(reward_all, group_all))
        loss = jnp.sum(row_part) / row_part.shape[0]
        return loss, lax.dynamic_slice_in_dim(logp, me * rows, rows), lax.dynamic_slice_in_dim(logp_ref, me * rows, rows)

    return jax.shard_map(device_step, mesh=mesh, in_specs=in_specs, out_specs=out_specs, check_vma=False)
```
